256 devices in a mesh: lon: 64 (over y, z, core), lev: 4 (over x).
Axes of the slice: x: 4, y: 4, z: 8, core: 2. Of those that a mesh axis runs over, the one named last changes fastest.
Arguments:
- column_old: float32 [70, 2097152], P(None, ('lon', 'lev')), may hold values from -6 to 6
- coupling: float32 [69, 2097152], P(None, ('lon', 'lev')), may hold values from 7.5 to 120, as said below
- sea_temp: float32 [2097152], P(('lon', 'lev')), may hold values from -6 to 6
- land_mask: int32 [2097152], P(('lon', 'lev')), may hold values from 0 to 1, as said below
- tile_weight: float32 [9, 2097152], P(None, ('lon', 'lev')), may hold values from 0.05 to 1
- tile_coeff: float32 [9, 2097152], P(None, ('lon', 'lev')), may hold values from 0.2 to 5
- tile_capacity: float32 [9, 2097152], P(None, ('lon', 'lev')), may hold values from 0.5 to 5
- tile_conduct: float32 [9, 2097152], P(None, ('lon', 'lev')), may hold values from 0.1 to 2
- tile_old: float32 [9, 2097152], P(None, ('lon', 'lev')), may hold values from -6 to 6
- tile_forcing: float32 [9, 2097152], P(None, ('lon', 'lev')), may hold values from -12 to 12
Outputs:
- column_temp: float32 [70, 2097152], P(None, ('lon', 'lev'))
- tile_temp: float32 [9, 2097152], P(None, ('lon', 'lev'))
The draws below stay inside these ranges and needn't reach their ends.
Inputs may be any that keep to these rules, and one draw needn't show every extreme that they name: `land_mask`: 1 marks a land column, 0 an ocean column. `coupling`: positive.
All inputs are finite; a program needn't handle non-finite values.
Results may differ from the reference program's by a relative error of at most 0.0001.
Values sent between devices are 32-bit elements; how exact they have to be, the bound alone decides.
A program may use at most 64 MiB of HBM per device.

```python
import math
import jax
import jax.numpy as jnp
from jax import lax

COLS_DEV = 8192
LEV = 70
NT = 9
ITERS = 8
COLUMNS = 2097152
N_LON = 64
N_LEV = 4


def draw_land_mask(key, part):
    first_key = jax.random.fold_in(key, 11)
    second_key = jax.random.fold_in(key, 12)
    blocks = COLUMNS // COLS_DEV
    land_level = jax.random.randint(first_key, (blocks, 1), 0, 9)
    column_roll = jax.random.randint(second_key, (blocks, COLS_DEV), 0, 8)
    return (column_roll < land_level).astype(jnp.int32).reshape(COLUMNS)


def draw_coupling(key, part):
    base_key = jax.random.fold_in(key, 21)
    rough_key = jax.random.fold_in(key, 22)
    tiles = COLUMNS // 128
    base_log = jax.random.uniform(base_key, (1, tiles), jnp.float32, math.log(15.0), math.log(60.0))
    base = jnp.repeat(jnp.exp(base_log), 128, axis=1)
    rough_log = jax.random.uniform(rough_key, (LEV - 1, COLUMNS), jnp.float32, math.log(0.5), math.log(2.0))
    rough = jnp.exp(rough_log)
    return (base * rough).astype(jnp.float32)


def block_levels(own_key, dims, shards, smallest, high):
    factor_of, own = 1.0, jax.random.fold_in(own_key, 6)
    for position, blocks in shards:
        draws = jnp.exp(jax.random.uniform(jax.random.fold_in(own, position), (blocks,), jnp.float32, smallest / len(shards), high / len(shards)))
        factor_of = factor_of * jnp.repeat(draws, dims[position] // blocks).reshape([-1 if axis == position else 1 for axis in range(len(dims))])
    return factor_of


def normal_values(key, shape, scale, bound, split=(), held_as=jnp.bfloat16):
    factor_of = block_levels(key, shape, split, -0.22, 0.18) if split else 1.0
    array = jax.random.normal(key, shape, jnp.float32) * scale * factor_of
    return jnp.minimum(jnp.maximum(array, -bound), bound).astype(held_as)


def setup_inputs(seed: int = 0) -> dict:
    key_of = jax.random.split(jax.random.key(seed), 11)
    column_old = normal_values(key_of[0], (LEV, COLUMNS), 1.0, 6.0, ((1, 256),), jnp.float32)
    coupling = draw_coupling(jax.random.fold_in(key_of[10], 71), 0)
    sea_temp = normal_values(key_of[2], (COLUMNS,), 1.0, 6.0, ((0, 256),), jnp.float32)
    land_mask = draw_land_mask(jax.random.fold_in(key_of[10], 71), 0)
    tile_weight = jnp.clip(jnp.exp(math.log(1.0) - 2.9957323 * jax.random.uniform(key_of[4], (NT, COLUMNS), jnp.float32) ** block_levels(key_of[4], (NT, COLUMNS), ((1, 256),), -0.2, 0.2)), 0.05, 1.0)
    tile_coeff = jnp.clip(jnp.exp(math.log(5.0) - 3.218876 * jax.random.uniform(key_of[5], (NT, COLUMNS), jnp.float32) ** block_levels(key_of[5], (NT, COLUMNS), ((1, 256),), -0.2, 0.2)), 0.2, 5.0)
    tile_capacity = jnp.clip(jnp.exp(math.log(5.0) - 2.3025851 * jax.random.uniform(key_of[6], (NT, COLUMNS), jnp.float32) ** block_levels(key_of[6], (NT, COLUMNS), ((1, 256),), -0.2, 0.2)), 0.5, 5.0)
    tile_conduct = jnp.clip(jnp.exp(math.log(2.0) - 2.9957323 * jax.random.uniform(key_of[7], (NT, COLUMNS), jnp.float32) ** block_levels(key_of[7], (NT, COLUMNS), ((1, 256),), -0.2, 0.2)), 0.1, 2.0)
    tile_old = normal_values(key_of[8], (NT, COLUMNS), 1.0, 6.0, ((1, 256),), jnp.float32)
    tile_forcing = normal_values(key_of[9], (NT, COLUMNS), 2.0, 12.0, ((1, 256),), jnp.float32)
    return {"column_old": column_old, "coupling": coupling, "sea_temp": sea_temp, "land_mask": land_mask, "tile_weight": tile_weight, "tile_coeff": tile_coeff, "tile_capacity": tile_capacity, "tile_conduct": tile_conduct, "tile_old": tile_old, "tile_forcing": tile_forcing}


def eliminate_upper(column_old, smooth):
    zero_row = jnp.zeros_like(smooth[:1])
    k_below = smooth[1:]
    k_above = jnp.concatenate([smooth[2:], zero_row], axis=0)

    def one_level(carried, layer_data):
        offset_next, factor_next = carried
        right_side, below_k, above_k = layer_data
        pivots = 1.0 + below_k + above_k - above_k * factor_next
        offset = (right_side + above_k * offset_next) / pivots
        factor = below_k / pivots
        return (offset, factor), (offset, factor)

    initial = (jnp.zeros_like(column_old[0]), jnp.zeros_like(column_old[0]))
    last, stacked = lax.scan(one_level, initial, (column_old[2:], k_below, k_above), reverse=True, unroll=4)
    return last[0], last[1], stacked[0], stacked[1]


def lower_levels(column_old, smooth, offset_two, factor_two, surface_flux):
    k_ground = smooth[0] * (1.0 + 0.5 * jnp.tanh(surface_flux))
    k_second = smooth[1]
    pivot_one = 1.0 + k_ground + k_second - k_second * factor_two
    offset_one = (column_old[1] + k_second * offset_two) / pivot_one
    factor_one = k_ground / pivot_one
    pivot_ground = 1.0 + k_ground - k_ground * factor_one
    return (column_old[0] + k_ground * offset_one) / pivot_ground, 1.0 / pivot_ground, offset_one, factor_one


def surface_solve(p_surf, q_surf, column_a, column_b):
    return (p_surf + q_surf * column_a) / (1.0 + q_surf * column_b)


def tile_sums(tile_weight, tile_coeff, tile_capacity, tile_conduct, tile_old, tile_forcing):
    fraction = tile_weight / jnp.sum(tile_weight, axis=0)
    denominator = tile_capacity + tile_coeff + tile_conduct
    source = tile_capacity * tile_old + tile_forcing
    land_a = jnp.sum(fraction * tile_coeff * source / denominator, axis=0)
    land_b = jnp.sum(fraction * tile_coeff * (tile_capacity + tile_conduct) / denominator, axis=0)
    return land_a, land_b, denominator, source


def substitute(surface, offset_one, factor_one, upper_offset, upper_factor):
    level_one = offset_one + factor_one * surface

    def one_level(below_value, layer_data):
        value = layer_data[0] + layer_data[1] * below_value
        return value, value

    unused, higher = lax.scan(one_level, level_one, (upper_offset, upper_factor), unroll=4)
    return jnp.concatenate([surface[None], level_one[None], higher], axis=0)


def reference(column_old, coupling, sea_temp, land_mask, tile_weight, tile_coeff, tile_capacity, tile_conduct, tile_old, tile_forcing):
    smooth = (jnp.roll(coupling, 1, axis=1) + 2.0 * coupling + jnp.roll(coupling, -1, axis=1)) * 0.25
    offset_two, factor_two, upper_offset, upper_factor = eliminate_upper(column_old, smooth)
    land_a, land_b, denominator, source = tile_sums(tile_weight, tile_coeff, tile_capacity, tile_conduct, tile_old, tile_forcing)
    blocks = N_LON * N_LEV
    slot_count = COLS_DEV // N_LON
    mask_blocks = land_mask.reshape(blocks, COLS_DEV)
    land_rank = (jnp.cumsum(mask_blocks, axis=1) - 1).astype(jnp.int32)
    device = jnp.arange(blocks, dtype=jnp.int32)[:, None]
    lon_source = device // N_LEV
    lev_source = device % N_LEV
    owner_block = (land_rank % N_LON) * N_LEV + lev_source
    land_place = owner_block * COLS_DEV + lon_source * slot_count + land_rank // N_LON
    land_place = jnp.where(mask_blocks == 1, land_place, COLUMNS).reshape(COLUMNS).astype(jnp.int32)
    land_fetch = jnp.clip(land_place, 0, COLUMNS - 1).astype(jnp.int32)
    is_land = land_mask == 1
    column_a = jnp.where(is_land, land_a[land_fetch], sea_temp)
    column_b = jnp.where(is_land, land_b[land_fetch], jnp.ones_like(sea_temp))
    surface_flux = jnp.zeros_like(sea_temp)
    surface = jnp.zeros_like(sea_temp)
    offset_one = jnp.zeros_like(sea_temp)
    factor_one = jnp.zeros_like(sea_temp)
    for repeat in range(ITERS):
        p_surf, q_surf, offset_one, factor_one = lower_levels(column_old, smooth, offset_two, factor_two, surface_flux)
        surface = surface_solve(p_surf, q_surf, column_a, column_b)
        surface_flux = column_a - column_b * surface
    land_surface = jnp.zeros_like(sea_temp).at[land_place].set(surface, mode="drop")
    tile_temp = (source + tile_coeff * land_surface) / denominator
    column_temp = substitute(surface, offset_one, factor_one, upper_offset, upper_factor)
    return column_temp, tile_temp
```

```python
import jax
import jax.numpy as jnp
from jax import lax
from jax.experimental import pallas as pl
from jax.experimental.pallas import tpu as pltpu
from jax.sharding import PartitionSpec as P

LEV = 70
NT = 9
COLS = 8192
ROWS = 64
LANES = 128
ITERS = 8
N_LON = 64
N_LEV = 4
MESH = pl.DeviceIdType.MESH
F32 = jnp.float32
BF16 = jnp.bfloat16
I32 = jnp.int32


def row(ref, level, start=0):
    return ref[pl.ds(level, 1), pl.ds(start, COLS)].reshape(ROWS, LANES)


def three_parts(value):
    high = value.astype(BF16)
    rest = value - high.astype(F32)
    middle = rest.astype(BF16)
    low = (rest - middle.astype(F32)).astype(BF16)
    return high, middle, low


def take(value, index):
    return jnp.take_along_axis(value, index, axis=1, mode="promise_in_bounds")


def flag(condition):
    return jnp.where(condition, 1.0, 0.0).astype(BF16)


def iota(shape, dim):
    return lax.broadcasted_iota(I32, shape, dim)


def peer_at(step, lon, sign=1):
    kz, ky, same_core = step // 8, (step // 2) % 4, step % 2
    dz = 4 + (kz // 2) * (1 - kz % 2) - ((kz + 1) // 2) * (kz % 2)
    dy = 2 + (ky // 2) * (1 - ky % 2) - ((ky + 1) // 2) * (ky % 2)
    y, z, core = lon // 16, (lon // 2) % 8, lon % 2
    return ((y + 4 + sign * dy) % 4) * 16 + ((z + 8 + sign * dz) % 8) * 2 + (core + 1 - same_core) % 2


def exchange(send, recv, send_sem, recv_sem, lon, lev):
    def copy(step, peer, landing):
        return pltpu.make_async_remote_copy(
            src_ref=send.at[pl.ds(peer, 1), :], dst_ref=recv.at[pl.ds(landing, 1), :],
            send_sem=send_sem.at[step], recv_sem=recv_sem.at[step],
            device_id={"lon": peer, "lev": lev}, device_id_type=MESH,
        )

    def start_one(step, carry):
        copy(step, peer_at(step, lon), lon).start()
        return carry

    def arrive_one(step, carry):
        copy(step, peer_at(step, lon), peer_at(step, lon, -1)).wait_recv()
        return carry

    def leave_one(step, carry):
        copy(step, peer_at(step, lon), lon).wait_send()
        return carry

    def loop(body):
        lax.fori_loop(0, N_LON - 1, body, 0, unroll=7)

    return lambda: loop(start_one), lambda: loop(arrive_one), lambda: loop(leave_one)


def kernel(
    col_h, cpl_h, sea_h, mask_h, w_h, co_h, ca_h, cd_h, old_h, fo_h,
    out_h, tile_h,
    col, cpl, es, fs, sea_s, mask_s, w_s, co_s, ca_s, cd_s, old_s, fo_s,
    scaled, coeff_r, tile_o, ab_send, ab_recv, back_send, back_recv,
    in_sem, halo_send_sem, halo_recv_sem, ab_send_sem, ab_recv_sem, back_send_sem, back_recv_sem,
    out_sem,
):
    lon, lev = lax.axis_index("lon"), lax.axis_index("lev")
    block = lon * N_LEV + lev
    right, left = (block + 1) % (N_LON * N_LEV), (block + N_LON * N_LEV - 1) % (N_LON * N_LEV)
    right_id = {"lon": right // N_LEV, "lev": right % N_LEV}
    left_id = {"lon": left // N_LEV, "lev": left % N_LEV}

    barrier = pltpu.get_barrier_semaphore()

    def greet(step, carry):
        pl.semaphore_signal(barrier, inc=1, device_id={"lon": peer_at(step, lon), "lev": lev}, device_id_type=MESH)
        return carry

    lax.fori_loop(0, N_LON - 1, greet, 0)
    for one in (left_id, right_id):
        pl.semaphore_signal(barrier, inc=1, device_id=one, device_id_type=MESH)

    own = cpl.at[:, pl.ds(LANES, COLS)]
    pairs = [
        (mask_h, mask_s), (w_h, w_s), (co_h, co_s), (ca_h, ca_s), (cd_h, cd_s), (old_h, old_s), (fo_h, fo_s),
        (cpl_h, own), (col_h, col), (sea_h, sea_s),
    ]
    loads = [pltpu.make_async_copy(src, dst, in_sem.at[n]) for n, (src, dst) in enumerate(pairs)]
    for load in loads:
        load.start()
    for load in loads[:7]:
        load.wait()

    weight_sum = sum_a = sum_b = None
    for tile in range(NT):
        weight, coeff = row(w_s, tile), row(co_s, tile)
        capacity, conduct = row(ca_s, tile), row(cd_s, tile)
        held = capacity + conduct
        inverse = 1.0 / (capacity + coeff + conduct)
        source = capacity * row(old_s, tile) + row(fo_s, tile)
        ratio = coeff * inverse
        scaled[tile] = source * inverse
        coeff_r[tile] = ratio
        share = weight * ratio
        weight_sum = weight if tile == 0 else weight_sum + weight
        sum_a = share * source if tile == 0 else sum_a + share * source
        sum_b = share * held if tile == 0 else sum_b + share * held
    whole = 1.0 / weight_sum
    ab_send[:, pl.ds(0, LANES)] = sum_a * whole
    ab_send[:, pl.ds(LANES, LANES)] = sum_b * whole
    loads[7].wait()

    pl.semaphore_wait(barrier, N_LON + 1)

    start_ab, arrive_ab, leave_ab = exchange(ab_send, ab_recv, ab_send_sem, ab_recv_sem, lon, lev)
    start_ab()
    halos = [
        pltpu.make_async_remote_copy(
            src_ref=cpl.at[:, pl.ds(COLS, LANES)], dst_ref=cpl.at[:, pl.ds(0, LANES)],
            send_sem=halo_send_sem.at[0], recv_sem=halo_recv_sem.at[0], device_id=right_id, device_id_type=MESH,
        ),
        pltpu.make_async_remote_copy(
            src_ref=cpl.at[:, pl.ds(LANES, LANES)], dst_ref=cpl.at[:, pl.ds(COLS + LANES, LANES)],
            send_sem=halo_send_sem.at[1], recv_sem=halo_recv_sem.at[1], device_id=left_id, device_id_type=MESH,
        ),
    ]
    for halo in halos:
        halo.start()
    ab_recv[pl.ds(lon, 1), :] = ab_send[pl.ds(lon, 1), :]

    lane = iota((ROWS, LANES), 1)
    is_land = mask_s[...] == 1
    land = flag(is_land)
    running = jnp.dot(land, flag(iota((LANES, LANES), 0) <= iota((LANES, LANES), 1)), preferred_element_type=F32)
    count = jnp.dot(land, jnp.ones((LANES, LANES), BF16), preferred_element_type=F32)
    before = jnp.dot(
        flag(iota((ROWS, ROWS), 1) < iota((ROWS, ROWS), 0)), count.astype(BF16), preferred_element_type=F32
    ).astype(I32)
    running, count = running.astype(I32), count.astype(I32)
    first_window, shift = before >> 6, before & 63
    windows = [flag(lane == first_window + n) for n in range(3)]
    place = shift + running - 1
    window_of, slot_a = place >> 6, place & 63
    slot_b = slot_a + 64
    lane_of = jnp.zeros((ROWS, LANES), I32)
    for half in (64, 32, 16, 8, 4, 2, 1):
        seen = take(running, lane_of + (half - 1))
        lane_of = jnp.where(seen <= lane, lane_of + half, lane_of)
    turned = (lane - shift) & 127
    lane_of = take(lane_of, turned)
    used = turned < count
    in_front, behind = used & (lane >= shift), used & (lane < shift)

    for halo in halos:
        halo.wait_recv()
    loads[8].wait()

    def smooth(level):
        centre, below, above = row(cpl, level, LANES), row(cpl, level), row(cpl, level, 2 * LANES)
        low = pltpu.roll(jnp.where(lane == LANES - 1, below, centre), 1, 1)
        high = pltpu.roll(jnp.where(lane == 0, above, centre), LANES - 1, 1)
        return (low + 2.0 * centre + high) * 0.25

    def eliminate(step, carried):
        k_here, offset, factor = carried
        for n in range(4):
            level = LEV - 1 - n - 4 * step
            k_below = smooth(level - 1)
            inverse = 1.0 / (1.0 + k_below + k_here - k_here * factor)
            offset = (row(col, level) + k_here * offset) * inverse
            factor = k_below * inverse
            es[level] = offset
            fs[level] = factor
            k_here = k_below
        return k_here, offset, factor

    zeros = jnp.zeros((ROWS, LANES), F32)
    k_second, offset_two, factor_two = lax.fori_loop(0, (LEV - 2) // 4, eliminate, (zeros, zeros, zeros))
    k_base = smooth(0)
    pivot_base = 1.0 + k_second - k_second * factor_two
    right_one = row(col, 1) + k_second * offset_two
    old_ground = row(col, 0)
    loads[9].wait()

    arrive_ab()
    both = jnp.concatenate([ab_recv[:, pl.ds(0, LANES)], ab_recv[:, pl.ds(LANES, LANES)]], axis=0)
    stacked = jnp.concatenate(windows, axis=0)
    picked = lax.dot_general(
        jnp.concatenate([stacked] * 3, axis=1), jnp.concatenate(three_parts(both), axis=1),
        (((1,), (1,)), ((), ())), preferred_element_type=F32,
    )
    pieces = [picked[n * ROWS : (n + 1) * ROWS] for n in range(3)]

    def unpack(slot):
        found = [take(piece, slot) for piece in pieces]
        return jnp.where(window_of == 0, found[0], jnp.where(window_of == 1, found[1], found[2]))

    column_a = jnp.where(is_land, unpack(slot_a), sea_s[...])
    column_b = jnp.where(is_land, unpack(slot_b), 1.0)

    flux = jnp.zeros((ROWS, LANES), F32)
    ground_a, one_b = old_ground + column_a, 1.0 + column_b
    for _ in range(ITERS):
        k_ground = k_base * (1.0 + 0.5 * jnp.tanh(flux))
        pivot_one = pivot_base + k_ground
        surface = (ground_a * pivot_one + k_ground * right_one) / (one_b * pivot_one + k_ground * pivot_base)
        flux = column_a - column_b * surface
    inverse = 1.0 / pivot_one
    offset_one, factor_one = right_one * inverse, k_ground * inverse

    ordered = take(surface, lane_of)
    packed = jnp.concatenate([jnp.where(in_front, ordered, 0.0), jnp.where(behind, ordered, 0.0)], axis=0).T
    targets = jnp.concatenate(
        [
            jnp.concatenate([windows[0], windows[2]], axis=0),
            jnp.concatenate([windows[1], jnp.zeros((ROWS, LANES), BF16)], axis=0),
        ],
        axis=1,
    )
    placed = jnp.dot(
        jnp.concatenate(three_parts(packed), axis=1), jnp.concatenate([targets] * 3, axis=0),
        preferred_element_type=F32,
    )
    back_send[...] = placed[:ROWS, :LANES] + placed[ROWS:, LANES:]

    start_back, arrive_back, leave_back = exchange(back_send, back_recv, back_send_sem, back_recv_sem, lon, lev)
    start_back()
    back_recv[pl.ds(lon, 1), :] = back_send[pl.ds(lon, 1), :]

    stores = []
    value = offset_one + factor_one * surface
    col[pl.ds(0, 1), :] = surface.reshape(1, COLS)
    col[pl.ds(1, 1), :] = value.reshape(1, COLS)
    for group in range(0, LEV, 8):
        count_here = min(8, LEV - group)
        for level in range(max(group, 2), group + count_here):
            value = es[level] + fs[level] * value
            col[pl.ds(level, 1), :] = value.reshape(1, COLS)
        part = pl.ds(group, count_here)
        store = pltpu.make_async_copy(col.at[part, :], out_h.at[part, :], out_sem.at[group // 8])
        store.start()
        stores.append(store)

    arrive_back()
    land_surface = back_recv[...]
    for tile in range(NT):
        tile_o[pl.ds(tile, 1), :] = (scaled[tile] + coeff_r[tile] * land_surface).reshape(1, COLS)
    store = pltpu.make_async_copy(tile_o, tile_h, out_sem.at[9])
    store.start()
    stores.append(store)
    for halo in halos:
        halo.wait_send()
    leave_ab()
    leave_back()
    for store in stores:
        store.wait()


def on_device(column_old, coupling, sea_temp, land_mask, *tiles):
    any_space = pl.BlockSpec(memory_space=pl.ANY)
    levels, tile_rows = pltpu.VMEM((LEV, COLS), F32), pltpu.VMEM((NT, COLS), F32)
    plane = pltpu.VMEM((ROWS, LANES), F32)
    return pl.pallas_call(
        kernel,
        out_shape=(jax.ShapeDtypeStruct((LEV, COLS), F32), jax.ShapeDtypeStruct((NT, COLS), F32)),
        in_specs=[any_space] * 10,
        out_specs=(any_space, any_space),
        scratch_shapes=[
            levels,
            pltpu.VMEM((LEV - 1, COLS + 2 * LANES), F32),
            pltpu.VMEM((LEV, ROWS, LANES), F32),
            pltpu.VMEM((LEV, ROWS, LANES), F32),
            plane,
            pltpu.VMEM((ROWS, LANES), I32),
            *[tile_rows] * 6,
            pltpu.VMEM((NT, ROWS, LANES), F32),
            pltpu.VMEM((NT, ROWS, LANES), F32),
            tile_rows,
            pltpu.VMEM((N_LON, 2 * LANES), F32),
            pltpu.VMEM((N_LON, 2 * LANES), F32),
            plane,
            plane,
            pltpu.SemaphoreType.DMA((10,)),
            pltpu.SemaphoreType.DMA((2,)),
            pltpu.SemaphoreType.DMA((2,)),
            *[pltpu.SemaphoreType.DMA((N_LON - 1,))] * 4,
            pltpu.SemaphoreType.DMA((10,)),
        ],
        compiler_params=pltpu.CompilerParams(collective_id=0, has_side_effects=True),
    )(column_old, coupling, sea_temp.reshape(ROWS, LANES), land_mask.reshape(ROWS, LANES), *tiles)


def solution(mesh):
    columns, lines = P(None, ("lon", "lev")), P(("lon", "lev"))
    return jax.shard_map(
        on_device,
        mesh=mesh,
        in_specs=(columns, columns, lines, lines) + (columns,) * 6,
        out_specs=(columns, columns),
        check_vma=False,
    )
```

```python
import jax
import jax.numpy as jnp
from jax import lax
from jax.experimental import pallas as pl
from jax.experimental.pallas import tpu as pltpu
from jax.sharding import PartitionSpec as P

LEV = 70
NT = 9
COLS = 8192
ROWS = 64
LANES = 128
ITERS = 8
N_LON = 64
N_LEV = 4
N_Y = 4
N_Z = 8
MESH = pl.DeviceIdType.MESH
F32 = jnp.float32
BF16 = jnp.bfloat16
I32 = jnp.int32


def row(ref, level, start=0):
    return ref[pl.ds(level, 1), pl.ds(start, COLS)].reshape(ROWS, LANES)


def two_parts(value):
    high = value.astype(BF16)
    return jnp.concatenate([high, (value - high.astype(F32)).astype(BF16)], axis=1)


def take(value, index):
    return jnp.take_along_axis(value, index, axis=1, mode="promise_in_bounds")


def flag(condition):
    return jnp.where(condition, 1.0, 0.0).astype(BF16)


def iota(shape, dim):
    return lax.broadcasted_iota(I32, shape, dim)


def away(step, length):
    return min(step, length - step)


OFFSETS = sorted(
    [(dy, dz, other) for dy in range(N_Y) for dz in range(N_Z) for other in range(2) if dy + dz + other],
    key=lambda step: -(2 * away(step[0], N_Y) + 2 * away(step[1], N_Z) + step[2]),
)


def neighbours(lon):
    y, z, core = lon // (2 * N_Z), (lon // 2) % N_Z, lon % 2
    at_y = [(y + step) % N_Y * (2 * N_Z) for step in range(N_Y)]
    at_z = [(z + step) % N_Z * 2 for step in range(N_Z)]
    at_core = [core, 1 - core]
    to = [at_y[dy] + at_z[dz] + at_core[other] for dy, dz, other in OFFSETS]
    back = [at_y[-dy % N_Y] + at_z[-dz % N_Z] + at_core[other] for dy, dz, other in OFFSETS]
    return to, back


def exchange(send, recv, send_sem, recv_sem, peers, lon, lev):
    def copy(step, landing):
        return pltpu.make_async_remote_copy(
            src_ref=send.at[pl.ds(peers[0][step], 1), :], dst_ref=recv.at[pl.ds(landing, 1), :],
            send_sem=send_sem.at[step], recv_sem=recv_sem.at[step],
            device_id={"lon": peers[0][step], "lev": lev}, device_id_type=MESH,
        )

    steps = range(N_LON - 1)
    return [copy(step, lon) for step in steps], [copy(step, peers[1][step]) for step in steps]


def solve(k_base, pivot_base, right_one, old_ground, column_a, column_b):
    flux = jnp.zeros_like(k_base)
    ground_a, one_b = old_ground + column_a, 1.0 + column_b
    for _ in range(ITERS):
        k_ground = k_base * (1.0 + 0.5 * jnp.tanh(flux))
        pivot_one = pivot_base + k_ground
        surface = (ground_a * pivot_one + k_ground * right_one) / (one_b * pivot_one + k_ground * pivot_base)
        flux = column_a - column_b * surface
    return surface, k_ground, pivot_one


def kernel(
    col_h, cpl_h, sea_h, mask_h, w_h, co_h, ca_h, cd_h, old_h, fo_h,
    out, land_out, scaled, coeff_r,
    col, cpl, ks, es, fs, sea_s, mask_s, w_s, co_s, ca_s, cd_s, old_s, fo_s,
    ab_send, ab_recv, to_land, from_columns,
    in_sem, halo_send_sem, halo_recv_sem, ab_send_sem, ab_recv_sem, land_send_sem, land_recv_sem,
):
    lon, lev = lax.axis_index("lon"), lax.axis_index("lev")
    block = lon * N_LEV + lev
    right, left = (block + 1) % (N_LON * N_LEV), (block + N_LON * N_LEV - 1) % (N_LON * N_LEV)
    right_id = {"lon": right // N_LEV, "lev": right % N_LEV}
    left_id = {"lon": left // N_LEV, "lev": left % N_LEV}

    own = cpl.at[:, pl.ds(LANES, COLS)]
    pairs = [
        (mask_h, mask_s), (w_h, w_s), (co_h, co_s), (ca_h, ca_s), (cd_h, cd_s), (old_h, old_s), (fo_h, fo_s),
        (cpl_h, own), (col_h, col), (sea_h, sea_s),
    ]
    loads = [pltpu.make_async_copy(src, dst, in_sem.at[n]) for n, (src, dst) in enumerate(pairs)]
    for load in loads:
        load.start()

    barrier = pltpu.get_barrier_semaphore()

    peers = neighbours(lon)
    for peer in peers[0]:
        pl.semaphore_signal(barrier, inc=1, device_id={"lon": peer, "lev": lev}, device_id_type=MESH)
    for one in (left_id, right_id):
        pl.semaphore_signal(barrier, inc=1, device_id=one, device_id_type=MESH)

    for load in loads[:7]:
        load.wait()

    weight_sum = sum_a = sum_b = None
    for tile in range(NT):
        weight, coeff = row(w_s, tile), row(co_s, tile)
        capacity, conduct = row(ca_s, tile), row(cd_s, tile)
        held = capacity + conduct
        inverse = 1.0 / (capacity + coeff + conduct)
        source = capacity * row(old_s, tile) + row(fo_s, tile)
        ratio = coeff * inverse
        scaled[tile] = source * inverse
        coeff_r[tile] = ratio
        share = weight * ratio
        weight_sum = weight if tile == 0 else weight_sum + weight
        sum_a = share * source if tile == 0 else sum_a + share * source
        sum_b = share * held if tile == 0 else sum_b + share * held
    whole = 1.0 / weight_sum
    ab_send[:, pl.ds(0, LANES)] = sum_a * whole
    ab_send[:, pl.ds(LANES, LANES)] = sum_b * whole
    lane = iota((ROWS, LANES), 1)
    is_land = mask_s[...] == 1
    land = flag(is_land)
    running = jnp.dot(land, flag(iota((LANES, LANES), 0) <= iota((LANES, LANES), 1)), preferred_element_type=F32)
    count = jnp.dot(land, jnp.ones((LANES, LANES), BF16), preferred_element_type=F32)
    before = jnp.dot(
        flag(iota((ROWS, ROWS), 1) < iota((ROWS, ROWS), 0)), count.astype(BF16), preferred_element_type=F32
    ).astype(I32)
    running, count = running.astype(I32), count.astype(I32)
    first_window, shift = before >> 6, before & 63
    windows = [flag(lane == first_window + n) for n in range(3)]
    place = shift + running - 1
    window_of, slot_a = place >> 6, place & 63
    slot_b = slot_a + 64
    lane_of = jnp.zeros((ROWS, LANES), I32)
    for half in (64, 32, 16, 8, 4, 2, 1):
        seen = take(running, lane_of + (half - 1))
        lane_of = jnp.where(seen <= lane, lane_of + half, lane_of)
    turned = (lane - shift) & 127
    lane_of = take(lane_of, turned)
    used = turned < count
    in_front, behind = used & (lane >= shift), used & (lane < shift)

    loads[7].wait()
    pl.semaphore_wait(barrier, N_LON + 1)

    halos = [
        pltpu.make_async_remote_copy(
            src_ref=cpl.at[:, pl.ds(COLS, LANES)], dst_ref=cpl.at[:, pl.ds(0, LANES)],
            send_sem=halo_send_sem.at[0], recv_sem=halo_recv_sem.at[0], device_id=right_id, device_id_type=MESH,
        ),
        pltpu.make_async_remote_copy(
            src_ref=cpl.at[:, pl.ds(LANES, LANES)], dst_ref=cpl.at[:, pl.ds(COLS + LANES, LANES)],
            send_sem=halo_send_sem.at[1], recv_sem=halo_recv_sem.at[1], device_id=left_id, device_id_type=MESH,
        ),
    ]
    ab_out, ab_in = exchange(ab_send, ab_recv, ab_send_sem, ab_recv_sem, peers, lon, lev)
    for copy in halos + ab_out:
        copy.start()
    ab_recv[pl.ds(lon, 1), :] = ab_send[pl.ds(lon, 1), :]

    lane_wide = iota((LEV - 1, LANES), 1)

    def smooth(chunk):
        below, centre, above = (cpl[:, pl.ds((chunk + n) * LANES, LANES)] for n in range(3))
        low = pltpu.roll(jnp.where(lane_wide == LANES - 1, below, centre), 1, 1)
        high = pltpu.roll(jnp.where(lane_wide == 0, above, centre), LANES - 1, 1)
        ks[:, pl.ds(chunk * LANES, LANES)] = (low + 2.0 * centre + high) * 0.25

    for chunk in range(1, ROWS - 1):
        smooth(chunk)
    def eliminate(first, carried, k_row, old_row, keep):
        k_here, offset, top, bottom = carried
        for n in range(4):
            level = first - n
            k_below = k_row(level - 1)
            part = k_below * bottom
            pivot = part + top
            inverse = 1.0 / pivot
            offset = (old_row(level) + k_here * offset) * (bottom * inverse)
            factor = part * inverse
            keep(level, offset, factor)
            k_here, top, bottom = k_below, pivot + k_below * top, pivot
        return (k_here, offset, top * inverse, jnp.ones_like(top)), factor

    def start_of(shape):
        zeros, ones = jnp.zeros(shape, F32), jnp.ones(shape, F32)
        return (zeros, zeros, ones, ones), zeros

    def keep_all(level, offset, factor):
        es[level] = offset
        fs[level] = factor

    def all_columns(step, carried):
        return eliminate(
            LEV - 1 - 4 * step, carried[0], lambda level: row(ks, level), lambda level: row(col, level), keep_all
        )

    ks[:, pl.ds(0, LANES)] = jnp.ones((LEV - 1, LANES), F32)
    ks[:, pl.ds(COLS - LANES, LANES)] = jnp.ones((LEV - 1, LANES), F32)
    loads[8].wait()
    inner, inner_factor = lax.fori_loop(0, (LEV - 2) // 4, all_columns, start_of((ROWS, LANES)))

    for halo in halos:
        halo.wait_recv()
    smooth(0)
    smooth(ROWS - 1)
    sublane = iota((8, LANES), 0)

    def edge_row(ref, level):
        low, high = (ref[pl.ds(level, 1), pl.ds(start, 8 * LANES)].reshape(8, LANES) for start in (0, COLS - 8 * LANES))
        return jnp.where(sublane == 0, low, high)

    def keep_edges(level, offset, factor):
        for ref, value in ((es, offset), (fs, factor)):
            ref[level, pl.ds(0, 1), :] = value[0:1]
            ref[level, pl.ds(ROWS - 1, 1), :] = value[7:8]

    def edge_columns(step, carried):
        return eliminate(
            LEV - 1 - 4 * step, carried[0], lambda level: edge_row(ks, level), lambda level: edge_row(col, level), keep_edges
        )

    edge, edge_factor = lax.fori_loop(0, (LEV - 2) // 4, edge_columns, start_of((8, LANES)))

    def joined(all_rows, edges):
        first = jnp.where(sublane == 0, edges, all_rows[0:8])
        last = jnp.where(sublane == 7, edges, all_rows[ROWS - 8 :])
        return jnp.concatenate([first, all_rows[8 : ROWS - 8], last], axis=0)

    k_second, offset_two, pivot_base = (joined(inner[n], edge[n]) for n in range(3))
    k_base = row(ks, 0)
    right_one = row(col, 1) + k_second * offset_two
    old_ground = row(col, 0)

    targets = jnp.concatenate(
        [
            jnp.concatenate([windows[0], windows[2]], axis=0),
            jnp.concatenate([windows[1], jnp.zeros((ROWS, LANES), BF16)], axis=0),
        ],
        axis=1,
    )
    fields = (k_base, pivot_base, right_one, old_ground)
    turned_fields = []
    for field in fields:
        ordered = take(field, lane_of)
        turned_fields.append(
            jnp.concatenate([jnp.where(in_front, ordered, 0.0), jnp.where(behind, ordered, 0.0)], axis=0).T
        )
    placed = jnp.dot(
        two_parts(jnp.concatenate(turned_fields, axis=0)), jnp.concatenate([targets] * 2, axis=0),
        preferred_element_type=F32,
    )
    for n in range(len(fields)):
        top = 2 * ROWS * n
        to_land[:, pl.ds(n * LANES, LANES)] = (
            placed[top : top + ROWS, :LANES] + placed[top + ROWS : top + 2 * ROWS, LANES:]
        )
    land_outgoing, land_incoming = exchange(to_land, from_columns, land_send_sem, land_recv_sem, peers, lon, lev)
    for copy in land_outgoing:
        copy.start()
    from_columns[pl.ds(lon, 1), :] = to_land[pl.ds(lon, 1), :]
    loads[9].wait()

    for copy in ab_in:
        copy.wait_recv()
    both = jnp.concatenate([ab_recv[:, pl.ds(0, LANES)], ab_recv[:, pl.ds(LANES, LANES)]], axis=0)
    stacked = jnp.concatenate(windows, axis=0)
    picked = lax.dot_general(
        jnp.concatenate([stacked] * 2, axis=1), two_parts(both),
        (((1,), (1,)), ((), ())), preferred_element_type=F32,
    )
    pieces = [picked[n * ROWS : (n + 1) * ROWS] for n in range(3)]

    def unpack(slot):
        found = [take(piece, slot) for piece in pieces]
        return jnp.where(window_of == 0, found[0], jnp.where(window_of == 1, found[1], found[2]))

    column_a = jnp.where(is_land, unpack(slot_a), sea_s[...])
    column_b = jnp.where(is_land, unpack(slot_b), 1.0)

    surface, k_ground, pivot_one = solve(*fields, column_a, column_b)
    inverse = 1.0 / pivot_one
    offset_one, factor_one = right_one * inverse, k_ground * inverse

    value = offset_one + factor_one * surface
    out[pl.ds(0, 1), :] = surface.reshape(1, COLS)
    out[pl.ds(1, 1), :] = value.reshape(1, COLS)
    for level in range(2, LEV):
        value = es[level] + fs[level] * value
        out[pl.ds(level, 1), :] = value.reshape(1, COLS)

    for copy in halos + ab_out + land_outgoing:
        copy.wait_send()
    for copy in land_incoming:
        copy.wait_recv()
    land_out[:, pl.ds(0, 4 * LANES)] = from_columns[...]
    land_out[:, pl.ds(4 * LANES, 2 * LANES)] = ab_send[...]


def finish(out, land, scaled, coeff_r, out_h, tile_h, tile_o, sems):
    stores = []
    for first in range(0, LEV, 8):
        part = pl.ds(first, min(8, LEV - first))
        stores.append(pltpu.make_async_copy(out.at[part, :], out_h.at[part, :], sems.at[1 + first // 8]))
        stores[-1].start()
    k_base, pivot_base, right_one, old_ground, land_a, land_b = (land[:, pl.ds(n * LANES, LANES)] for n in range(6))
    taken = pivot_base > 0.0
    surface, _, _ = solve(k_base, jnp.where(taken, pivot_base, 1.0), right_one, old_ground, land_a, land_b)
    land_surface = jnp.where(taken, surface, 0.0)
    for tile in range(NT):
        tile_o[pl.ds(tile, 1), :] = (scaled[tile] + coeff_r[tile] * land_surface).reshape(1, COLS)
    stores.append(pltpu.make_async_copy(tile_o, tile_h, sems.at[0]))
    stores[-1].start()
    for store in stores:
        store.wait()


def on_device(column_old, coupling, sea_temp, land_mask, *tiles):
    any_space = pl.BlockSpec(memory_space=pl.ANY)
    levels, tile_rows = pltpu.VMEM((LEV, COLS), F32), pltpu.VMEM((NT, COLS), F32)
    plane = pltpu.VMEM((ROWS, LANES), F32)
    in_vmem = pl.BlockSpec(memory_space=pltpu.VMEM)
    arrays = (column_old, coupling, sea_temp.reshape(ROWS, LANES), land_mask.reshape(ROWS, LANES), *tiles)
    tile_planes = pltpu.VMEM((NT, ROWS, LANES), F32)
    results = pl.pallas_call(
        kernel,
        out_shape=(levels, pltpu.VMEM((ROWS, 6 * LANES), F32), tile_planes, tile_planes),
        in_specs=[any_space] * 10,
        out_specs=(in_vmem,) * 4,
        scratch_shapes=[
            levels,
            pltpu.VMEM((LEV - 1, COLS + 2 * LANES), F32),
            pltpu.VMEM((LEV - 1, COLS), F32),
            pltpu.VMEM((LEV, ROWS, LANES), F32),
            pltpu.VMEM((LEV, ROWS, LANES), F32),
            plane,
            pltpu.VMEM((ROWS, LANES), I32),
            *[tile_rows] * 6,
            *[pltpu.VMEM((N_LON, 2 * LANES), F32)] * 2,
            *[pltpu.VMEM((N_LON, 4 * LANES), F32)] * 2,
            pltpu.SemaphoreType.DMA((10,)),
            pltpu.SemaphoreType.DMA((2,)),
            pltpu.SemaphoreType.DMA((2,)),
            *[pltpu.SemaphoreType.DMA((N_LON - 1,))] * 4,
        ],
        compiler_params=pltpu.CompilerParams(
            collective_id=0, has_side_effects=True, vmem_limit_bytes=24 * 2**20
        ),
    )(*[pltpu.with_memory_space_constraint(array, pltpu.HBM) for array in arrays])
    return pl.pallas_call(
        finish,
        out_shape=(jax.ShapeDtypeStruct((LEV, COLS), F32), jax.ShapeDtypeStruct((NT, COLS), F32)),
        in_specs=[in_vmem] * 4,
        out_specs=(any_space, any_space),
        scratch_shapes=[tile_rows, pltpu.SemaphoreType.DMA((10,))],
        compiler_params=pltpu.CompilerParams(vmem_limit_bytes=4 * 2**20),
    )(*results)


def solution(mesh):
    columns, lines = P(None, ("lon", "lev")), P(("lon", "lev"))
    return jax.shard_map(
        on_device,
        mesh=mesh,
        in_specs=(columns, columns, lines, lines) + (columns,) * 6,
        out_specs=(columns, columns),
        check_vma=False,
    )
```

```python
import jax
import jax.numpy as jnp
from jax import lax
from jax.experimental import pallas as pl
from jax.experimental.pallas import tpu as pltpu
from jax.sharding import PartitionSpec as P

LEV = 70
NT = 9
COLS = 8192
ROWS = 64
LANES = 128
ITERS = 8
N_LON = 64
N_LEV = 4
N_Y = 4
N_Z = 8
MESH = pl.DeviceIdType.MESH
F32 = jnp.float32
BF16 = jnp.bfloat16
I32 = jnp.int32


def row(ref, level, start=0):
    return ref[pl.ds(level, 1), pl.ds(start, COLS)].reshape(ROWS, LANES)


def two_parts(value):
    high = value.astype(BF16)
    return jnp.concatenate([high, (value - high.astype(F32)).astype(BF16)], axis=1)


def take(value, index):
    return jnp.take_along_axis(value, index, axis=1, mode="promise_in_bounds")


def flag(condition):
    return jnp.where(condition, 1.0, 0.0).astype(BF16)


def iota(shape, dim):
    return lax.broadcasted_iota(I32, shape, dim)


def away(step, length):
    return min(step, length - step)


OFFSETS = sorted(
    [(dy, dz, other) for dy in range(N_Y) for dz in range(N_Z) for other in range(2) if dy + dz + other],
    key=lambda step: -(2 * away(step[0], N_Y) + 2 * away(step[1], N_Z) + step[2]),
)


def neighbours(lon):
    y, z, core = lon // (2 * N_Z), (lon // 2) % N_Z, lon % 2
    at_y = [(y + step) % N_Y * (2 * N_Z) for step in range(N_Y)]
    at_z = [(z + step) % N_Z * 2 for step in range(N_Z)]
    at_core = [core, 1 - core]
    return [at_y[dy] + at_z[dz] + at_core[other] for dy, dz, other in OFFSETS]


def exchange(send, recv, total, sems, peers, lon, lev):
    copies = [
        pltpu.make_async_remote_copy(
            src_ref=send.at[pl.ds(peer, 1), :], dst_ref=recv.at[pl.ds(lon, 1), :], send_sem=sems.at[0], recv_sem=sems.at[1],
            device_id={"lon": peer, "lev": lev}, device_id_type=MESH,
        )
        for peer in peers
    ]
    return copies, pltpu.make_async_remote_copy(
        src_ref=total, dst_ref=total, send_sem=sems.at[0], recv_sem=sems.at[1],
        device_id={"lon": peers[0], "lev": lev}, device_id_type=MESH,
    )


def solve(k_base, pivot_base, right_one, old_ground, column_a, column_b):
    flux = jnp.zeros_like(k_base)
    ground_a, one_b = old_ground + column_a, 1.0 + column_b
    for _ in range(ITERS):
        k_ground = k_base * (1.0 + 0.5 * jnp.tanh(flux))
        pivot_one = pivot_base + k_ground
        surface = (ground_a * pivot_one + k_ground * right_one) / (one_b * pivot_one + k_ground * pivot_base)
        flux = column_a - column_b * surface
    return surface, k_ground, pivot_one


def kernel(
    col_h, cpl_h, sea_h, mask_h, w_h, co_h, ca_h, cd_h, old_h, fo_h,
    out, land_out, scaled, coeff_r,
    col, cpl, ks, es, fs, sea_s, mask_s, w_s, co_s, ca_s, cd_s, old_s, fo_s,
    ab_send, ab_recv, to_land, from_columns,
    ab_total, land_total, in_sem, halo_send_sem, halo_recv_sem, ab_sems, land_sems,
):
    lon, lev = lax.axis_index("lon"), lax.axis_index("lev")
    block = lon * N_LEV + lev
    right, left = (block + 1) % (N_LON * N_LEV), (block + N_LON * N_LEV - 1) % (N_LON * N_LEV)
    right_id = {"lon": right // N_LEV, "lev": right % N_LEV}
    left_id = {"lon": left // N_LEV, "lev": left % N_LEV}

    own = cpl.at[:, pl.ds(LANES, COLS)]
    pairs = [
        (co_h, co_s), (ca_h, ca_s), (cd_h, cd_s), (old_h, old_s), (fo_h, fo_s), (w_h, w_s), (cpl_h, own), (mask_h, mask_s),
        (col_h, col), (sea_h, sea_s),
    ]
    loads = [pltpu.make_async_copy(src, dst, in_sem.at[n]) for n, (src, dst) in enumerate(pairs)]
    for load in loads:
        load.start()

    barrier = pltpu.get_barrier_semaphore()

    for one in (left_id, right_id):
        pl.semaphore_signal(barrier, inc=1, device_id=one, device_id_type=MESH)
    peers = neighbours(lon)
    for peer in peers:
        pl.semaphore_signal(barrier, inc=1, device_id={"lon": peer, "lev": lev}, device_id_type=MESH)

    for load in loads[:6]:
        load.wait()

    weight_sum = sum_a = sum_b = None
    for tile in range(NT):
        weight, coeff = row(w_s, tile), row(co_s, tile)
        capacity, conduct = row(ca_s, tile), row(cd_s, tile)
        held = capacity + conduct
        inverse = 1.0 / (capacity + coeff + conduct)
        source = capacity * row(old_s, tile) + row(fo_s, tile)
        ratio = coeff * inverse
        scaled[tile] = source * inverse
        coeff_r[tile] = ratio
        share = weight * ratio
        weight_sum = weight if tile == 0 else weight_sum + weight
        sum_a = share * source if tile == 0 else sum_a + share * source
        sum_b = share * held if tile == 0 else sum_b + share * held
    whole = 1.0 / weight_sum
    ab_send[:, pl.ds(0, LANES)] = sum_a * whole
    ab_send[:, pl.ds(LANES, LANES)] = sum_b * whole
    loads[6].wait()
    pl.semaphore_wait(barrier, N_LON + 1)

    halos = [
        pltpu.make_async_remote_copy(
            src_ref=cpl.at[:, pl.ds(COLS, LANES)], dst_ref=cpl.at[:, pl.ds(0, LANES)],
            send_sem=halo_send_sem.at[0], recv_sem=halo_recv_sem.at[0], device_id=right_id, device_id_type=MESH,
        ),
        pltpu.make_async_remote_copy(
            src_ref=cpl.at[:, pl.ds(LANES, LANES)], dst_ref=cpl.at[:, pl.ds(COLS + LANES, LANES)],
            send_sem=halo_send_sem.at[1], recv_sem=halo_recv_sem.at[1], device_id=left_id, device_id_type=MESH,
        ),
    ]
    for halo in halos:
        halo.start()
    ab_out, ab_all = exchange(ab_send, ab_recv, ab_total, ab_sems, peers, lon, lev)
    for copy in ab_out:
        copy.start()
    ab_recv[pl.ds(lon, 1), :] = ab_send[pl.ds(lon, 1), :]

    lane = iota((ROWS, LANES), 1)
    loads[7].wait()
    is_land = mask_s[...] == 1
    land = flag(is_land)
    running = jnp.dot(land, flag(iota((LANES, LANES), 0) <= iota((LANES, LANES), 1)), preferred_element_type=F32)
    count = jnp.dot(land, jnp.ones((LANES, LANES), BF16), preferred_element_type=F32)
    before = jnp.dot(
        flag(iota((ROWS, ROWS), 1) < iota((ROWS, ROWS), 0)), count.astype(BF16), preferred_element_type=F32
    ).astype(I32)
    running, count = running.astype(I32), count.astype(I32)
    first_window, shift = before >> 6, before & 63
    windows = [flag(lane == first_window + n) for n in range(3)]
    place = shift + running - 1
    window_of, slot_a = place >> 6, place & 63
    slot_b = slot_a + 64
    lane_of = jnp.zeros((ROWS, LANES), I32)
    for half in (64, 32, 16, 8, 4, 2, 1):
        seen = take(running, lane_of + (half - 1))
        lane_of = jnp.where(seen <= lane, lane_of + half, lane_of)
    turned = (lane - shift) & 127
    lane_of = take(lane_of, turned)
    used = turned < count
    in_front, behind = used & (lane >= shift), used & (lane < shift)

    lane_wide = iota((LEV - 1, LANES), 1)

    def smooth(chunk):
        below, centre, above = (cpl[:, pl.ds((chunk + n) * LANES, LANES)] for n in range(3))
        low = pltpu.roll(jnp.where(lane_wide == LANES - 1, below, centre), 1, 1)
        high = pltpu.roll(jnp.where(lane_wide == 0, above, centre), LANES - 1, 1)
        ks[:, pl.ds(chunk * LANES, LANES)] = (low + 2.0 * centre + high) * 0.25

    for chunk in range(1, ROWS - 1):
        smooth(chunk)
    def eliminate(first, carried, k_row, old_row, keep):
        k_here, offset, top, bottom = carried
        for n in range(4):
            level = first - n
            k_below = k_row(level - 1)
            part = k_below * bottom
            pivot = part + top
            inverse = 1.0 / pivot
            offset = (old_row(level) + k_here * offset) * (bottom * inverse)
            factor = part * inverse
            keep(level, offset, factor)
            k_here, top, bottom = k_below, pivot + k_below * top, pivot
        return (k_here, offset, top * inverse, jnp.ones_like(top)), factor

    def start_of(shape):
        zeros, ones = jnp.zeros(shape, F32), jnp.ones(shape, F32)
        return (zeros, zeros, ones, ones), zeros

    def keep_all(level, offset, factor):
        es[level] = offset
        fs[level] = factor

    def all_columns(step, carried):
        return eliminate(
            LEV - 1 - 4 * step, carried[0], lambda level: row(ks, level), lambda level: row(col, level), keep_all
        )

    ks[:, pl.ds(0, LANES)] = jnp.ones((LEV - 1, LANES), F32)
    ks[:, pl.ds(COLS - LANES, LANES)] = jnp.ones((LEV - 1, LANES), F32)
    loads[8].wait()
    inner, inner_factor = lax.fori_loop(0, (LEV - 2) // 4, all_columns, start_of((ROWS, LANES)))

    for halo in halos:
        halo.wait_recv()
    smooth(0)
    smooth(ROWS - 1)
    sublane = iota((8, LANES), 0)

    def edge_row(ref, level):
        low, high = (ref[pl.ds(level, 1), pl.ds(start, 8 * LANES)].reshape(8, LANES) for start in (0, COLS - 8 * LANES))
        return jnp.where(sublane == 0, low, high)

    def keep_edges(level, offset, factor):
        for ref, value in ((es, offset), (fs, factor)):
            ref[level, pl.ds(0, 1), :] = value[0:1]
            ref[level, pl.ds(ROWS - 1, 1), :] = value[7:8]

    def edge_columns(step, carried):
        return eliminate(
            LEV - 1 - 4 * step, carried[0], lambda level: edge_row(ks, level), lambda level: edge_row(col, level), keep_edges
        )

    edge, edge_factor = lax.fori_loop(0, (LEV - 2) // 4, edge_columns, start_of((8, LANES)))

    def joined(all_rows, edges):
        first = jnp.where(sublane == 0, edges, all_rows[0:8])
        last = jnp.where(sublane == 7, edges, all_rows[ROWS - 8 :])
        return jnp.concatenate([first, all_rows[8 : ROWS - 8], last], axis=0)

    k_second, offset_two, pivot_base = (joined(inner[n], edge[n]) for n in range(3))
    k_base = row(ks, 0)
    right_one = row(col, 1) + k_second * offset_two
    old_ground = row(col, 0)

    targets = jnp.concatenate(
        [
            jnp.concatenate([windows[0], windows[2]], axis=0),
            jnp.concatenate([windows[1], jnp.zeros((ROWS, LANES), BF16)], axis=0),
        ],
        axis=1,
    )
    fields = (k_base, pivot_base, right_one, old_ground)
    turned_fields = []
    for field in fields:
        ordered = take(field, lane_of)
        turned_fields.append(
            jnp.concatenate([jnp.where(in_front, ordered, 0.0), jnp.where(behind, ordered, 0.0)], axis=0).T
        )
    placed = jnp.dot(
        two_parts(jnp.concatenate(turned_fields, axis=0)), jnp.concatenate([targets] * 2, axis=0),
        preferred_element_type=F32,
    )
    for n in range(len(fields)):
        top = 2 * ROWS * n
        to_land[:, pl.ds(n * LANES, LANES)] = (
            placed[top : top + ROWS, :LANES] + placed[top + ROWS : top + 2 * ROWS, LANES:]
        )
    land_outgoing, land_all = exchange(to_land, from_columns, land_total, land_sems, peers, lon, lev)
    for copy in land_outgoing:
        copy.start()
    from_columns[pl.ds(lon, 1), :] = to_land[pl.ds(lon, 1), :]
    loads[9].wait()

    ab_all.wait_recv()
    both = jnp.concatenate([ab_recv[:, pl.ds(0, LANES)], ab_recv[:, pl.ds(LANES, LANES)]], axis=0)
    stacked = jnp.concatenate(windows, axis=0)
    picked = lax.dot_general(
        jnp.concatenate([stacked] * 2, axis=1), two_parts(both),
        (((1,), (1,)), ((), ())), preferred_element_type=F32,
    )
    pieces = [picked[n * ROWS : (n + 1) * ROWS] for n in range(3)]

    def unpack(slot):
        found = [take(piece, slot) for piece in pieces]
        return jnp.where(window_of == 0, found[0], jnp.where(window_of == 1, found[1], found[2]))

    column_a = jnp.where(is_land, unpack(slot_a), sea_s[...])
    column_b = jnp.where(is_land, unpack(slot_b), 1.0)

    surface, k_ground, pivot_one = solve(*fields, column_a, column_b)
    inverse = 1.0 / pivot_one
    offset_one, factor_one = right_one * inverse, k_ground * inverse

    value = offset_one + factor_one * surface
    out[pl.ds(0, 1), :] = surface.reshape(1, COLS)
    out[pl.ds(1, 1), :] = value.reshape(1, COLS)
    for level in range(2, LEV):
        value = es[level] + fs[level] * value
        out[pl.ds(level, 1), :] = value.reshape(1, COLS)

    for copy in (*halos, ab_all, land_all):
        copy.wait_send()
    land_all.wait_recv()
    land_out[:, pl.ds(0, 4 * LANES)] = from_columns[...]
    land_out[:, pl.ds(4 * LANES, 2 * LANES)] = ab_send[...]


def finish(out, land, scaled, coeff_r, out_h, tile_h, tile_o, sems):
    stores = []
    for first in range(0, LEV, 8):
        part = pl.ds(first, min(8, LEV - first))
        stores.append(pltpu.make_async_copy(out.at[part, :], out_h.at[part, :], sems.at[1 + first // 8]))
        stores[-1].start()
    k_base, pivot_base, right_one, old_ground, land_a, land_b = (land[:, pl.ds(n * LANES, LANES)] for n in range(6))
    taken = pivot_base > 0.0
    surface, _, _ = solve(k_base, jnp.where(taken, pivot_base, 1.0), right_one, old_ground, land_a, land_b)
    land_surface = jnp.where(taken, surface, 0.0)
    for tile in range(NT):
        tile_o[pl.ds(tile, 1), :] = (scaled[tile] + coeff_r[tile] * land_surface).reshape(1, COLS)
    stores.append(pltpu.make_async_copy(tile_o, tile_h, sems.at[0]))
    stores[-1].start()
    for store in stores:
        store.wait()


def on_device(column_old, coupling, sea_temp, land_mask, *tiles):
    any_space = pl.BlockSpec(memory_space=pl.ANY)
    levels, tile_rows = pltpu.VMEM((LEV, COLS), F32), pltpu.VMEM((NT, COLS), F32)
    plane = pltpu.VMEM((ROWS, LANES), F32)
    in_vmem = pl.BlockSpec(memory_space=pltpu.VMEM)
    arrays = (column_old, coupling, sea_temp.reshape(ROWS, LANES), land_mask.reshape(ROWS, LANES), *tiles)
    tile_planes = pltpu.VMEM((NT, ROWS, LANES), F32)
    results = pl.pallas_call(
        kernel,
        out_shape=(levels, pltpu.VMEM((ROWS, 6 * LANES), F32), tile_planes, tile_planes),
        in_specs=[any_space] * 10,
        out_specs=(in_vmem,) * 4,
        scratch_shapes=[
            levels,
            pltpu.VMEM((LEV - 1, COLS + 2 * LANES), F32),
            pltpu.VMEM((LEV - 1, COLS), F32),
            pltpu.VMEM((LEV, ROWS, LANES), F32),
            pltpu.VMEM((LEV, ROWS, LANES), F32),
            plane,
            pltpu.VMEM((ROWS, LANES), I32),
            *[tile_rows] * 6,
            *[pltpu.VMEM((N_LON, 2 * LANES), F32)] * 2,
            *[pltpu.VMEM((N_LON, 4 * LANES), F32)] * 2,
            pltpu.VMEM(((N_LON - 1) * 2, LANES), F32),
            pltpu.VMEM(((N_LON - 1) * 4, LANES), F32),
            pltpu.SemaphoreType.DMA((10,)),
            pltpu.SemaphoreType.DMA((2,)),
            pltpu.SemaphoreType.DMA((2,)),
            pltpu.SemaphoreType.DMA((2,)),
            pltpu.SemaphoreType.DMA((2,)),
        ],
        compiler_params=pltpu.CompilerParams(
            collective_id=0, has_side_effects=True, vmem_limit_bytes=24 * 2**20
        ),
    )(*[pltpu.with_memory_space_constraint(array, pltpu.HBM) for array in arrays])
    return pl.pallas_call(
        finish,
        out_shape=(jax.ShapeDtypeStruct((LEV, COLS), F32), jax.ShapeDtypeStruct((NT, COLS), F32)),
        in_specs=[in_vmem] * 4,
        out_specs=(any_space, any_space),
        scratch_shapes=[tile_rows, pltpu.SemaphoreType.DMA((10,))],
        compiler_params=pltpu.CompilerParams(vmem_limit_bytes=4 * 2**20),
    )(*results)


def solution(mesh):
    columns, lines = P(None, ("lon", "lev")), P(("lon", "lev"))
    return jax.shard_map(
        on_device,
        mesh=mesh,
        in_specs=(columns, columns, lines, lines) + (columns,) * 6,
        out_specs=(columns, columns),
        check_vma=False,
    )
```

```python
import jax
import jax.numpy as jnp
from jax import lax
from jax.experimental import pallas as pl
from jax.experimental.pallas import tpu as pltpu
from jax.sharding import PartitionSpec as P

LEV = 70
NT = 9
COLS = 8192
ROWS = 64
LANES = 128
ITERS = 8
N_LON = 64
N_LEV = 4
N_Y = 4
N_Z = 8
MESH = pl.DeviceIdType.MESH
F32 = jnp.float32
BF16 = jnp.bfloat16
I32 = jnp.int32


def row(ref, level, start=0):
    return ref[pl.ds(level, 1), pl.ds(start, COLS)].reshape(ROWS, LANES)


def two_parts(value):
    high = value.astype(BF16)
    return jnp.concatenate([high, (value - high.astype(F32)).astype(BF16)], axis=1)


def take(value, index):
    return jnp.take_along_axis(value, index, axis=1, mode="promise_in_bounds")


def flag(condition):
    return jnp.where(condition, 1.0, 0.0).astype(BF16)


def iota(shape, dim):
    return lax.broadcasted_iota(I32, shape, dim)


def away(step, length):
    return min(step, length - step)


OFFSETS = sorted(
    [(dy, dz, other) for dy in range(N_Y) for dz in range(N_Z) for other in range(2) if dy + dz + other],
    key=lambda step: -(2 * away(step[0], N_Y) + 2 * away(step[1], N_Z) + step[2]),
)


def neighbours(lon):
    y, z, core = lon // (2 * N_Z), (lon // 2) % N_Z, lon % 2
    at_y = [(y + step) % N_Y * (2 * N_Z) for step in range(N_Y)]
    at_z = [(z + step) % N_Z * 2 for step in range(N_Z)]
    at_core = [core, 1 - core]
    return [at_y[dy] + at_z[dz] + at_core[other] for dy, dz, other in OFFSETS]


def exchange(send, recv, total, sems, peers, lon, lev):
    copies = [
        pltpu.make_async_remote_copy(
            src_ref=send.at[pl.ds(peer, 1), :], dst_ref=recv.at[pl.ds(lon, 1), :], send_sem=sems.at[0], recv_sem=sems.at[1],
            device_id={"lon": peer, "lev": lev}, device_id_type=MESH,
        )
        for peer in peers
    ]
    return copies, pltpu.make_async_remote_copy(
        src_ref=total, dst_ref=total, send_sem=sems.at[0], recv_sem=sems.at[1],
        device_id={"lon": peers[0], "lev": lev}, device_id_type=MESH,
    )


def solve(k_base, pivot_base, right_one, old_ground, column_a, column_b):
    flux = jnp.zeros_like(k_base)
    ground_a, one_b = old_ground + column_a, 1.0 + column_b
    for _ in range(ITERS):
        k_ground = k_base * (1.0 + 0.5 * jnp.tanh(flux))
        pivot_one = pivot_base + k_ground
        surface = (ground_a * pivot_one + k_ground * right_one) / (one_b * pivot_one + k_ground * pivot_base)
        flux = column_a - column_b * surface
    return surface, k_ground, pivot_one


def kernel(
    col_h, cpl_h, sea_h, mask_h, w_h, co_h, ca_h, cd_h, old_h, fo_h,
    out, land_out, scaled, coeff_r,
    col, cpl, ks, es, fs, sea_s, mask_s, w_s, co_s, ca_s, cd_s, old_s, fo_s,
    ab_send, ab_recv, to_land, from_columns,
    ab_total, land_total, in_sem, halo_send_sem, halo_recv_sem, ab_sems, land_sems,
):
    lon, lev = lax.axis_index("lon"), lax.axis_index("lev")
    block = lon * N_LEV + lev
    right, left = (block + 1) % (N_LON * N_LEV), (block + N_LON * N_LEV - 1) % (N_LON * N_LEV)
    right_id = {"lon": right // N_LEV, "lev": right % N_LEV}
    left_id = {"lon": left // N_LEV, "lev": left % N_LEV}

    own = cpl.at[:, pl.ds(LANES, COLS)]
    pairs = [
        (co_h, co_s), (ca_h, ca_s), (cd_h, cd_s), (old_h, old_s), (fo_h, fo_s), (w_h, w_s), (cpl_h, own), (mask_h, mask_s),
        (col_h, col), (sea_h, sea_s),
    ]
    loads = [pltpu.make_async_copy(src, dst, in_sem.at[n]) for n, (src, dst) in enumerate(pairs)]
    for load in loads:
        load.start()

    barrier = pltpu.get_barrier_semaphore()

    for one in (left_id, right_id):
        pl.semaphore_signal(barrier, inc=1, device_id=one, device_id_type=MESH)
    peers = neighbours(lon)
    for peer in peers:
        pl.semaphore_signal(barrier, inc=1, device_id={"lon": peer, "lev": lev}, device_id_type=MESH)

    for load in loads[:6]:
        load.wait()

    weight_sum = sum_a = sum_b = None
    for tile in range(NT):
        weight, coeff = row(w_s, tile), row(co_s, tile)
        capacity, conduct = row(ca_s, tile), row(cd_s, tile)
        held = capacity + conduct
        inverse = 1.0 / (capacity + coeff + conduct)
        source = capacity * row(old_s, tile) + row(fo_s, tile)
        ratio = coeff * inverse
        scaled[tile] = source * inverse
        coeff_r[tile] = ratio
        share = weight * ratio
        weight_sum = weight if tile == 0 else weight_sum + weight
        sum_a = share * source if tile == 0 else sum_a + share * source
        sum_b = share * held if tile == 0 else sum_b + share * held
    whole = 1.0 / weight_sum
    ab_send[:, pl.ds(0, LANES)] = sum_a * whole
    ab_send[:, pl.ds(LANES, LANES)] = sum_b * whole
    loads[6].wait()
    pl.semaphore_wait(barrier, N_LON + 1)

    halos = [
        pltpu.make_async_remote_copy(
            src_ref=cpl.at[:, pl.ds(COLS, LANES)], dst_ref=cpl.at[:, pl.ds(0, LANES)],
            send_sem=halo_send_sem.at[0], recv_sem=halo_recv_sem.at[0], device_id=right_id, device_id_type=MESH,
        ),
        pltpu.make_async_remote_copy(
            src_ref=cpl.at[:, pl.ds(LANES, LANES)], dst_ref=cpl.at[:, pl.ds(COLS + LANES, LANES)],
            send_sem=halo_send_sem.at[1], recv_sem=halo_recv_sem.at[1], device_id=left_id, device_id_type=MESH,
        ),
    ]
    for halo in halos:
        halo.start()
    ab_out, ab_all = exchange(ab_send, ab_recv, ab_total, ab_sems, peers, lon, lev)
    for copy in ab_out:
        copy.start()
    ab_recv[pl.ds(lon, 1), :] = ab_send[pl.ds(lon, 1), :]

    lane = iota((ROWS, LANES), 1)
    loads[7].wait()
    is_land = mask_s[...] == 1
    land = flag(is_land)
    running = jnp.dot(land, flag(iota((LANES, LANES), 0) <= iota((LANES, LANES), 1)), preferred_element_type=F32)
    count = jnp.dot(land, jnp.ones((LANES, LANES), BF16), preferred_element_type=F32)
    before = jnp.dot(
        flag(iota((ROWS, ROWS), 1) < iota((ROWS, ROWS), 0)), count.astype(BF16), preferred_element_type=F32
    ).astype(I32)
    running, count = running.astype(I32), count.astype(I32)
    first_window, shift = before >> 6, before & 63
    windows = [flag(lane == first_window + n) for n in range(3)]
    place = shift + running - 1
    window_of, slot_a = place >> 6, place & 63
    slot_b = slot_a + 64
    lane_of = jnp.zeros((ROWS, LANES), I32)
    for half in (64, 32, 16, 8, 4, 2, 1):
        seen = take(running, lane_of + (half - 1))
        lane_of = jnp.where(seen <= lane, lane_of + half, lane_of)
    turned = (lane - shift) & 127
    lane_of = take(lane_of, turned)
    used = turned < count
    in_front, behind = used & (lane >= shift), used & (lane < shift)
    line = iota((ROWS, LANES), 0)
    last = jnp.broadcast_to((before + count)[ROWS - 1 :, :], (ROWS, LANES)) - 1
    last_flag = jnp.broadcast_to(mask_s[pl.ds(ROWS - 1, 1), :][:, LANES - 1 :], (ROWS, LANES))
    first_column, last_column = (line == 0) & (lane == 0), (line == ROWS - 1) & (lane == LANES - 1)
    first_slot = first_column & is_land
    last_slot = (line == (last & 63)) & (lane == (last >> 6)) & (last_flag == 1)

    lane_wide = iota((LEV - 1, LANES), 1)

    def smooth(chunk, under=0, over=2):
        below, centre, above = (cpl[:, pl.ds((chunk + n) * LANES, LANES)] for n in (under, 1, over))
        low = pltpu.roll(jnp.where(lane_wide == LANES - 1, below, centre), 1, 1)
        high = pltpu.roll(jnp.where(lane_wide == 0, above, centre), LANES - 1, 1)
        ks[:, pl.ds(chunk * LANES, LANES)] = (low + 2.0 * centre + high) * 0.25

    smooth(0, under=1)
    smooth(ROWS - 1, over=1)
    for chunk in range(1, ROWS - 1):
        smooth(chunk)
    def eliminate(level, carried, k_row, old_row, keep):
        k_here, offset, top, bottom = carried
        k_below = k_row(level - 1)
        part = k_below * bottom
        pivot = part + top
        inverse = 1.0 / pivot
        offset = (old_row(level) + k_here * offset) * (bottom * inverse)
        keep(level, offset, part * inverse)
        return (k_below, offset, part + (1.0 + k_below) * top, pivot), inverse

    def scaled_down(carried, inverse):
        k_here, offset, top, _ = carried
        return k_here, offset, top * inverse, jnp.ones_like(top)

    def start_of(shape):
        zeros, ones = jnp.zeros(shape, F32), jnp.ones(shape, F32)
        return zeros, zeros, ones, ones

    def keep_all(level, offset, factor):
        es[level] = offset
        fs[level] = factor

    def all_columns(step, carried):
        for n in range(4):
            carried, inverse = eliminate(
                LEV - 1 - 4 * step - n, carried, lambda level: row(ks, level), lambda level: row(col, level), keep_all
            )
        return scaled_down(carried, inverse)

    loads[8].wait()
    k_second, offset_two, pivot_base, _ = lax.fori_loop(0, (LEV - 2) // 4, all_columns, start_of((ROWS, LANES)))
    fields = [row(ks, 0), pivot_base, row(col, 1) + k_second * offset_two, row(col, 0)]

    targets = jnp.concatenate(
        [
            jnp.concatenate([windows[0], windows[2]], axis=0),
            jnp.concatenate([windows[1], jnp.zeros((ROWS, LANES), BF16)], axis=0),
        ],
        axis=1,
    )
    turned_fields = []
    for field in fields:
        ordered = take(jnp.where(first_column | last_column, 0.0, field), lane_of)
        turned_fields.append(
            jnp.concatenate([jnp.where(in_front, ordered, 0.0), jnp.where(behind, ordered, 0.0)], axis=0).T
        )
    placed = jnp.dot(
        two_parts(jnp.concatenate(turned_fields, axis=0)), jnp.concatenate([targets] * 2, axis=0),
        preferred_element_type=F32,
    )
    for n in range(len(fields)):
        top = 2 * ROWS * n
        to_land[:, pl.ds(n * LANES, LANES)] = (
            placed[top : top + ROWS, :LANES] + placed[top + ROWS : top + 2 * ROWS, LANES:]
        )

    for halo in halos:
        halo.wait_recv()
    smooth(0)
    smooth(ROWS - 1)
    sublane = iota((8, LANES), 0)

    def edge_row(ref, level):
        low, high = (ref[pl.ds(level, 1), pl.ds(start, 8 * LANES)].reshape(8, LANES) for start in (0, COLS - 8 * LANES))
        return jnp.where(sublane == 0, low, high)

    def keep_edges(level, offset, factor):
        for ref, value in ((es, offset), (fs, factor)):
            ref[level, pl.ds(0, 1), :] = value[0:1]
            ref[level, pl.ds(ROWS - 1, 1), :] = value[7:8]

    edge = start_of((8, LANES))
    for level in range(LEV - 1, 1, -1):
        edge, inverse = eliminate(
            level, edge, lambda level: edge_row(ks, level), lambda level: edge_row(col, level), keep_edges
        )
        if level % 12 == 2:
            edge = scaled_down(edge, inverse)
    edge_fields = [edge_row(ks, 0), edge[2], edge_row(col, 1) + edge[0] * edge[1], edge_row(col, 0)]

    for n, value in enumerate(edge_fields):
        part = pl.ds(n * LANES, LANES)
        first_value, last_value = value[0:1, 0:1], value[7:8, LANES - 1 :]
        to_land[:, part] = jnp.where(first_slot, first_value, jnp.where(last_slot, last_value, to_land[:, part]))
    land_outgoing, land_all = exchange(to_land, from_columns, land_total, land_sems, peers, lon, lev)
    for copy in land_outgoing:
        copy.start()
    from_columns[pl.ds(lon, 1), :] = to_land[pl.ds(lon, 1), :]
    loads[9].wait()

    def joined(all_rows, edges):
        first = jnp.where(sublane == 0, edges, all_rows[0:8])
        last_rows = jnp.where(sublane == 7, edges, all_rows[ROWS - 8 :])
        return jnp.concatenate([first, all_rows[8 : ROWS - 8], last_rows], axis=0)

    fields = [joined(field, edges) for field, edges in zip(fields, edge_fields)]
    right_one = fields[2]

    ab_all.wait_recv()
    both = jnp.concatenate([ab_recv[:, pl.ds(0, LANES)], ab_recv[:, pl.ds(LANES, LANES)]], axis=0)
    stacked = jnp.concatenate(windows, axis=0)
    picked = lax.dot_general(
        jnp.concatenate([stacked] * 2, axis=1), two_parts(both),
        (((1,), (1,)), ((), ())), preferred_element_type=F32,
    )
    pieces = [picked[n * ROWS : (n + 1) * ROWS] for n in range(3)]

    def unpack(slot):
        found = [take(piece, slot) for piece in pieces]
        return jnp.where(window_of == 0, found[0], jnp.where(window_of == 1, found[1], found[2]))

    column_a = jnp.where(is_land, unpack(slot_a), sea_s[...])
    column_b = jnp.where(is_land, unpack(slot_b), 1.0)

    surface, k_ground, pivot_one = solve(*fields, column_a, column_b)
    inverse = 1.0 / pivot_one
    offset_one, factor_one = right_one * inverse, k_ground * inverse

    value = offset_one + factor_one * surface
    out[pl.ds(0, 1), :] = surface.reshape(1, COLS)
    out[pl.ds(1, 1), :] = value.reshape(1, COLS)
    for level in range(2, LEV):
        value = es[level] + fs[level] * value
        out[pl.ds(level, 1), :] = value.reshape(1, COLS)

    for copy in (*halos, ab_all, land_all):
        copy.wait_send()
    land_all.wait_recv()
    land_out[:, pl.ds(0, 4 * LANES)] = from_columns[...]
    land_out[:, pl.ds(4 * LANES, 2 * LANES)] = ab_send[...]


def finish(out, land, scaled, coeff_r, out_h, tile_h, tile_o, sems):
    stores = [pltpu.make_async_copy(out, out_h, sems.at[0]), pltpu.make_async_copy(tile_o, tile_h, sems.at[1])]
    stores[0].start()
    k_base, pivot_base, right_one, old_ground, land_a, land_b = (land[:, pl.ds(n * LANES, LANES)] for n in range(6))
    taken = pivot_base > 0.0
    surface, _, _ = solve(k_base, jnp.where(taken, pivot_base, 1.0), right_one, old_ground, land_a, land_b)
    land_surface = jnp.where(taken, surface, 0.0)
    for tile in range(NT):
        tile_o[pl.ds(tile, 1), :] = (scaled[tile] + coeff_r[tile] * land_surface).reshape(1, COLS)
    stores[1].start()
    for store in stores:
        store.wait()


def on_device(column_old, coupling, sea_temp, land_mask, *tiles):
    any_space = pl.BlockSpec(memory_space=pl.ANY)
    levels, tile_rows = pltpu.VMEM((LEV, COLS), F32), pltpu.VMEM((NT, COLS), F32)
    plane = pltpu.VMEM((ROWS, LANES), F32)
    in_vmem = pl.BlockSpec(memory_space=pltpu.VMEM)
    arrays = (column_old, coupling, sea_temp.reshape(ROWS, LANES), land_mask.reshape(ROWS, LANES), *tiles)
    tile_planes = pltpu.VMEM((NT, ROWS, LANES), F32)
    results = pl.pallas_call(
        kernel,
        out_shape=(levels, pltpu.VMEM((ROWS, 6 * LANES), F32), tile_planes, tile_planes),
        in_specs=[any_space] * 10,
        out_specs=(in_vmem,) * 4,
        scratch_shapes=[
            levels,
            pltpu.VMEM((LEV - 1, COLS + 2 * LANES), F32),
            pltpu.VMEM((LEV - 1, COLS), F32),
            pltpu.VMEM((LEV, ROWS, LANES), F32),
            pltpu.VMEM((LEV, ROWS, LANES), F32),
            plane,
            pltpu.VMEM((ROWS, LANES), I32),
            *[tile_rows] * 6,
            *[pltpu.VMEM((N_LON, 2 * LANES), F32)] * 2,
            *[pltpu.VMEM((N_LON, 4 * LANES), F32)] * 2,
            pltpu.VMEM(((N_LON - 1) * 2, LANES), F32),
            pltpu.VMEM(((N_LON - 1) * 4, LANES), F32),
            pltpu.SemaphoreType.DMA((10,)),
            pltpu.SemaphoreType.DMA((2,)),
            pltpu.SemaphoreType.DMA((2,)),
            pltpu.SemaphoreType.DMA((2,)),
            pltpu.SemaphoreType.DMA((2,)),
        ],
        compiler_params=pltpu.CompilerParams(
            collective_id=0, has_side_effects=True, vmem_limit_bytes=24 * 2**20
        ),
    )(*[pltpu.with_memory_space_constraint(array, pltpu.HBM) for array in arrays])
    return pl.pallas_call(
        finish,
        out_shape=(jax.ShapeDtypeStruct((LEV, COLS), F32), jax.ShapeDtypeStruct((NT, COLS), F32)),
        in_specs=[in_vmem] * 4,
        out_specs=(any_space, any_space),
        scratch_shapes=[tile_rows, pltpu.SemaphoreType.DMA((2,))],
        compiler_params=pltpu.CompilerParams(vmem_limit_bytes=4 * 2**20),
    )(*results)


def solution(mesh):
    columns, lines = P(None, ("lon", "lev")), P(("lon", "lev"))
    return jax.shard_map(
        on_device,
        mesh=mesh,
        in_specs=(columns, columns, lines, lines) + (columns,) * 6,
        out_specs=(columns, columns),
        check_vma=False,
    )
```

```python
import jax
import jax.numpy as jnp
from jax import lax
from jax.experimental import pallas as pl
from jax.experimental.pallas import tpu as pltpu
from jax.sharding import PartitionSpec as P

LEV = 70
NT = 9
COLS = 8192
ROWS = 64
LANES = 128
ITERS = 8
N_LON = 64
N_LEV = 4
N_Y = 4
N_Z = 8
MESH = pl.DeviceIdType.MESH
F32 = jnp.float32
BF16 = jnp.bfloat16
I32 = jnp.int32


def row(ref, level, start=0):
    return ref[pl.ds(level, 1), pl.ds(start, COLS)].reshape(ROWS, LANES)


def two_parts(value):
    high = value.astype(BF16)
    return jnp.concatenate([high, (value - high.astype(F32)).astype(BF16)], axis=1)


def take(value, index):
    return jnp.take_along_axis(value, index, axis=1, mode="promise_in_bounds")


def flag(condition):
    return jnp.where(condition, 1.0, 0.0).astype(BF16)


def iota(shape, dim):
    return lax.broadcasted_iota(I32, shape, dim)


def away(step, length):
    return min(step, length - step)


OFFSETS = sorted(
    [(dy, dz, other) for dy in range(N_Y) for dz in range(N_Z) for other in range(2) if dy + dz + other],
    key=lambda step: -(2 * away(step[0], N_Y) + 2 * away(step[1], N_Z) + step[2]),
)


def neighbours(lon):
    y, z, core = lon // (2 * N_Z), (lon // 2) % N_Z, lon % 2
    at_y = [(y + step) % N_Y * (2 * N_Z) for step in range(N_Y)]
    at_z = [(z + step) % N_Z * 2 for step in range(N_Z)]
    at_core = [core, 1 - core]
    return lambda dy, dz, other: at_y[dy] + at_z[dz] + at_core[other]


def exchange(send, recv, total, sems, peers, lon, lev):
    copies = [
        pltpu.make_async_remote_copy(
            src_ref=send.at[pl.ds(peer, 1), :], dst_ref=recv.at[pl.ds(lon, 1), :], send_sem=sems.at[0], recv_sem=sems.at[1],
            device_id={"lon": peer, "lev": lev}, device_id_type=MESH,
        )
        for peer in peers
    ]
    return copies, pltpu.make_async_remote_copy(
        src_ref=total, dst_ref=total, send_sem=sems.at[0], recv_sem=sems.at[1],
        device_id={"lon": peers[0], "lev": lev}, device_id_type=MESH,
    )


def solve(k_base, pivot_base, right_one, old_ground, column_a, column_b):
    flux = jnp.zeros_like(k_base)
    ground_a, one_b = old_ground + column_a, 1.0 + column_b
    for _ in range(ITERS):
        k_ground = k_base * (1.0 + 0.5 * jnp.tanh(flux))
        pivot_one = pivot_base + k_ground
        surface = (ground_a * pivot_one + k_ground * right_one) / (one_b * pivot_one + k_ground * pivot_base)
        flux = column_a - column_b * surface
    return surface, k_ground, pivot_one


def kernel(
    col_h, cpl_h, sea_h, mask_h, w_h, co_h, ca_h, cd_h, old_h, fo_h,
    out, land_out, scaled, coeff_r,
    col, cpl, ks, es, fs, sea_s, mask_s, w_s, co_s, ca_s, cd_s, old_s, fo_s,
    ab_send, ab_recv, to_land, from_columns,
    ab_total, land_total, in_sem, halo_send_sem, halo_recv_sem, ab_sems, land_sems, heard,
):
    lon, lev = lax.axis_index("lon"), lax.axis_index("lev")
    block = lon * N_LEV + lev
    right, left = (block + 1) % (N_LON * N_LEV), (block + N_LON * N_LEV - 1) % (N_LON * N_LEV)
    right_id = {"lon": right // N_LEV, "lev": right % N_LEV}
    left_id = {"lon": left // N_LEV, "lev": left % N_LEV}

    own = cpl.at[:, pl.ds(LANES, COLS)]
    pairs = [
        (mask_h, mask_s), (co_h, co_s), (ca_h, ca_s), (cd_h, cd_s), (old_h, old_s), (fo_h, fo_s), (w_h, w_s), (cpl_h, own),
        (col_h, col), (sea_h, sea_s),
    ]
    loads = [pltpu.make_async_copy(src, dst, in_sem.at[n]) for n, (src, dst) in enumerate(pairs)]
    for load in loads:
        load.start()

    barrier = pltpu.get_barrier_semaphore()

    for one in (left_id, right_id):
        pl.semaphore_signal(barrier, inc=1, device_id=one, device_id_type=MESH)
    at = neighbours(lon)
    peers = [at(*offset) for offset in OFFSETS]
    ring = [at(*offset) for offset in OFFSETS if offset[0] == 0]
    rows_y = [at(step, 0, 0) for step in range(1, N_Y)]

    def tell(semaphore, device):
        pl.semaphore_signal(semaphore, inc=1, device_id={"lon": device, "lev": lev}, device_id_type=MESH)

    for device in ring + rows_y:
        tell(barrier, device)

    lane = iota((ROWS, LANES), 1)
    loads[0].wait()
    is_land = mask_s[...] == 1
    land = flag(is_land)
    running = jnp.dot(land, flag(iota((LANES, LANES), 0) <= iota((LANES, LANES), 1)), preferred_element_type=F32)
    count = jnp.dot(land, jnp.ones((LANES, LANES), BF16), preferred_element_type=F32)
    before = jnp.dot(
        flag(iota((ROWS, ROWS), 1) < iota((ROWS, ROWS), 0)), count.astype(BF16), preferred_element_type=F32
    ).astype(I32)
    running, count = running.astype(I32), count.astype(I32)
    first_window, shift = before >> 6, before & 63
    windows = [flag(lane == first_window + n) for n in range(3)]
    place = shift + running - 1
    window_of, slot_a = place >> 6, place & 63
    slot_b = slot_a + 64
    lane_of = jnp.zeros((ROWS, LANES), I32)
    for half in (64, 32, 16, 8, 4, 2, 1):
        seen = take(running, lane_of + (half - 1))
        lane_of = jnp.where(seen <= lane, lane_of + half, lane_of)
    turned = (lane - shift) & 127
    lane_of = take(lane_of, turned)
    used = turned < count
    in_front, behind = used & (lane >= shift), used & (lane < shift)
    line = iota((ROWS, LANES), 0)
    last = jnp.broadcast_to((before + count)[ROWS - 1 :, :], (ROWS, LANES)) - 1
    last_flag = jnp.broadcast_to(mask_s[pl.ds(ROWS - 1, 1), :][:, LANES - 1 :], (ROWS, LANES))
    first_column, last_column = (line == 0) & (lane == 0), (line == ROWS - 1) & (lane == LANES - 1)
    first_slot = first_column & is_land
    last_slot = (line == (last & 63)) & (lane == (last >> 6)) & (last_flag == 1)

    for load in loads[1:7]:
        load.wait()

    weight_sum = sum_a = sum_b = None
    for tile in range(NT):
        weight, coeff = row(w_s, tile), row(co_s, tile)
        capacity, conduct = row(ca_s, tile), row(cd_s, tile)
        held = capacity + conduct
        inverse = 1.0 / (capacity + coeff + conduct)
        source = capacity * row(old_s, tile) + row(fo_s, tile)
        ratio = coeff * inverse
        scaled[tile] = source * inverse
        coeff_r[tile] = ratio
        share = weight * ratio
        weight_sum = weight if tile == 0 else weight_sum + weight
        sum_a = share * source if tile == 0 else sum_a + share * source
        sum_b = share * held if tile == 0 else sum_b + share * held
    whole = 1.0 / weight_sum
    ab_send[:, pl.ds(0, LANES)] = sum_a * whole
    ab_send[:, pl.ds(LANES, LANES)] = sum_b * whole
    loads[7].wait()
    pl.semaphore_wait(barrier, len(ring) + len(rows_y) + 2)

    halos = [
        pltpu.make_async_remote_copy(
            src_ref=cpl.at[:, pl.ds(COLS, LANES)], dst_ref=cpl.at[:, pl.ds(0, LANES)],
            send_sem=halo_send_sem.at[0], recv_sem=halo_recv_sem.at[0], device_id=right_id, device_id_type=MESH,
        ),
        pltpu.make_async_remote_copy(
            src_ref=cpl.at[:, pl.ds(LANES, LANES)], dst_ref=cpl.at[:, pl.ds(COLS + LANES, LANES)],
            send_sem=halo_send_sem.at[1], recv_sem=halo_recv_sem.at[1], device_id=left_id, device_id_type=MESH,
        ),
    ]
    for halo in halos:
        halo.start()
    for step, device in enumerate(rows_y):
        tell(heard.at[step], device)

    lane_wide = iota((LEV - 1, LANES), 1)

    def smooth(chunk, under=0, over=2):
        below, centre, above = (cpl[:, pl.ds((chunk + n) * LANES, LANES)] for n in (under, 1, over))
        low = pltpu.roll(jnp.where(lane_wide == LANES - 1, below, centre), 1, 1)
        high = pltpu.roll(jnp.where(lane_wide == 0, above, centre), LANES - 1, 1)
        ks[:, pl.ds(chunk * LANES, LANES)] = (low + 2.0 * centre + high) * 0.25

    smooth(0, under=1)
    smooth(ROWS - 1, over=1)
    for chunk in range(1, ROWS - 1):
        smooth(chunk)
    for step in range(len(rows_y)):
        pl.semaphore_wait(heard.at[step], 1)
    ab_out, ab_all = exchange(ab_send, ab_recv, ab_total, ab_sems, peers, lon, lev)
    for copy in ab_out:
        copy.start()
    ab_recv[pl.ds(lon, 1), :] = ab_send[pl.ds(lon, 1), :]

    def eliminate(level, carried, k_row, old_row, keep):
        k_here, offset, top, bottom = carried
        k_below = k_row(level - 1)
        part = k_below * bottom
        pivot = part + top
        inverse = 1.0 / pivot
        offset = (old_row(level) + k_here * offset) * (bottom * inverse)
        keep(level, offset, part * inverse)
        return (k_below, offset, part + (1.0 + k_below) * top, pivot), inverse

    def scaled_down(carried, inverse):
        k_here, offset, top, _ = carried
        return k_here, offset, top * inverse, jnp.ones_like(top)

    def start_of(shape):
        zeros, ones = jnp.zeros(shape, F32), jnp.ones(shape, F32)
        return zeros, zeros, ones, ones

    def keep_all(level, offset, factor):
        es[level] = offset
        fs[level] = factor

    def all_columns(step, carried):
        for n in range(4):
            carried, inverse = eliminate(
                LEV - 1 - 4 * step - n, carried, lambda level: row(ks, level), lambda level: row(col, level), keep_all
            )
        return scaled_down(carried, inverse)

    loads[8].wait()
    k_second, offset_two, pivot_base, _ = lax.fori_loop(0, (LEV - 2) // 4, all_columns, start_of((ROWS, LANES)))
    fields = [row(ks, 0), pivot_base, row(col, 1) + k_second * offset_two, row(col, 0)]

    targets = jnp.concatenate(
        [
            jnp.concatenate([windows[0], windows[2]], axis=0),
            jnp.concatenate([windows[1], jnp.zeros((ROWS, LANES), BF16)], axis=0),
        ],
        axis=1,
    )
    turned_fields = []
    for field in fields:
        ordered = take(jnp.where(first_column | last_column, 0.0, field), lane_of)
        turned_fields.append(
            jnp.concatenate([jnp.where(in_front, ordered, 0.0), jnp.where(behind, ordered, 0.0)], axis=0).T
        )
    placed = jnp.dot(
        two_parts(jnp.concatenate(turned_fields, axis=0)), jnp.concatenate([targets] * 2, axis=0),
        preferred_element_type=F32,
    )
    for n in range(len(fields)):
        top = 2 * ROWS * n
        to_land[:, pl.ds(n * LANES, LANES)] = (
            placed[top : top + ROWS, :LANES] + placed[top + ROWS : top + 2 * ROWS, LANES:]
        )

    for halo in halos:
        halo.wait_recv()
    smooth(0)
    smooth(ROWS - 1)
    sublane = iota((8, LANES), 0)

    def edge_row(ref, level):
        low, high = (ref[pl.ds(level, 1), pl.ds(start, 8 * LANES)].reshape(8, LANES) for start in (0, COLS - 8 * LANES))
        return jnp.where(sublane == 0, low, high)

    def keep_edges(level, offset, factor):
        for ref, value in ((es, offset), (fs, factor)):
            ref[level, pl.ds(0, 1), :] = value[0:1]
            ref[level, pl.ds(ROWS - 1, 1), :] = value[7:8]

    edge = start_of((8, LANES))
    for level in range(LEV - 1, 1, -1):
        edge, inverse = eliminate(
            level, edge, lambda level: edge_row(ks, level), lambda level: edge_row(col, level), keep_edges
        )
        if level % 12 == 2:
            edge = scaled_down(edge, inverse)
    edge_fields = [edge_row(ks, 0), edge[2], edge_row(col, 1) + edge[0] * edge[1], edge_row(col, 0)]

    for n, value in enumerate(edge_fields):
        part = pl.ds(n * LANES, LANES)
        first_value, last_value = value[0:1, 0:1], value[7:8, LANES - 1 :]
        to_land[:, part] = jnp.where(first_slot, first_value, jnp.where(last_slot, last_value, to_land[:, part]))
    land_outgoing, land_all = exchange(to_land, from_columns, land_total, land_sems, peers, lon, lev)
    for copy in land_outgoing:
        copy.start()
    from_columns[pl.ds(lon, 1), :] = to_land[pl.ds(lon, 1), :]
    loads[9].wait()

    def joined(all_rows, edges):
        first = jnp.where(sublane == 0, edges, all_rows[0:8])
        last_rows = jnp.where(sublane == 7, edges, all_rows[ROWS - 8 :])
        return jnp.concatenate([first, all_rows[8 : ROWS - 8], last_rows], axis=0)

    fields = [joined(field, edges) for field, edges in zip(fields, edge_fields)]
    right_one = fields[2]

    ab_all.wait_recv()
    both = jnp.concatenate([ab_recv[:, pl.ds(0, LANES)], ab_recv[:, pl.ds(LANES, LANES)]], axis=0)
    stacked = jnp.concatenate(windows, axis=0)
    picked = lax.dot_general(
        jnp.concatenate([stacked] * 2, axis=1), two_parts(both),
        (((1,), (1,)), ((), ())), preferred_element_type=F32,
    )
    pieces = [picked[n * ROWS : (n + 1) * ROWS] for n in range(3)]

    def unpack(slot):
        found = [take(piece, slot) for piece in pieces]
        return jnp.where(window_of == 0, found[0], jnp.where(window_of == 1, found[1], found[2]))

    column_a = jnp.where(is_land, unpack(slot_a), sea_s[...])
    column_b = jnp.where(is_land, unpack(slot_b), 1.0)

    surface, k_ground, pivot_one = solve(*fields, column_a, column_b)
    inverse = 1.0 / pivot_one
    offset_one, factor_one = right_one * inverse, k_ground * inverse

    value = offset_one + factor_one * surface
    out[pl.ds(0, 1), :] = surface.reshape(1, COLS)
    out[pl.ds(1, 1), :] = value.reshape(1, COLS)
    for level in range(2, LEV):
        value = es[level] + fs[level] * value
        out[pl.ds(level, 1), :] = value.reshape(1, COLS)

    for copy in (*halos, ab_all, land_all):
        copy.wait_send()
    land_all.wait_recv()
    land_out[:, pl.ds(0, 4 * LANES)] = from_columns[...]
    land_out[:, pl.ds(4 * LANES, 2 * LANES)] = ab_send[...]


def finish(out, land, scaled, coeff_r, out_h, tile_h, tile_o, sems):
    stores = [pltpu.make_async_copy(out, out_h, sems.at[0]), pltpu.make_async_copy(tile_o, tile_h, sems.at[1])]
    stores[0].start()
    k_base, pivot_base, right_one, old_ground, land_a, land_b = (land[:, pl.ds(n * LANES, LANES)] for n in range(6))
    taken = pivot_base > 0.0
    surface, _, _ = solve(k_base, jnp.where(taken, pivot_base, 1.0), right_one, old_ground, land_a, land_b)
    land_surface = jnp.where(taken, surface, 0.0)
    for tile in range(NT):
        tile_o[pl.ds(tile, 1), :] = (scaled[tile] + coeff_r[tile] * land_surface).reshape(1, COLS)
    stores[1].start()
    for store in stores:
        store.wait()


def on_device(column_old, coupling, sea_temp, land_mask, *tiles):
    any_space = pl.BlockSpec(memory_space=pl.ANY)
    levels, tile_rows = pltpu.VMEM((LEV, COLS), F32), pltpu.VMEM((NT, COLS), F32)
    plane = pltpu.VMEM((ROWS, LANES), F32)
    in_vmem = pl.BlockSpec(memory_space=pltpu.VMEM)
    arrays = (column_old, coupling, sea_temp.reshape(ROWS, LANES), land_mask.reshape(ROWS, LANES), *tiles)
    tile_planes = pltpu.VMEM((NT, ROWS, LANES), F32)
    results = pl.pallas_call(
        kernel,
        out_shape=(levels, pltpu.VMEM((ROWS, 6 * LANES), F32), tile_planes, tile_planes),
        in_specs=[any_space] * 10,
        out_specs=(in_vmem,) * 4,
        scratch_shapes=[
            levels,
            pltpu.VMEM((LEV - 1, COLS + 2 * LANES), F32),
            pltpu.VMEM((LEV - 1, COLS), F32),
            pltpu.VMEM((LEV, ROWS, LANES), F32),
            pltpu.VMEM((LEV, ROWS, LANES), F32),
            plane,
            pltpu.VMEM((ROWS, LANES), I32),
            *[tile_rows] * 6,
            *[pltpu.VMEM((N_LON, 2 * LANES), F32)] * 2,
            *[pltpu.VMEM((N_LON, 4 * LANES), F32)] * 2,
            pltpu.VMEM(((N_LON - 1) * 2, LANES), F32),
            pltpu.VMEM(((N_LON - 1) * 4, LANES), F32),
            pltpu.SemaphoreType.DMA((10,)),
            pltpu.SemaphoreType.DMA((2,)),
            pltpu.SemaphoreType.DMA((2,)),
            pltpu.SemaphoreType.DMA((2,)),
            pltpu.SemaphoreType.DMA((2,)),
            pltpu.SemaphoreType.REGULAR((N_Y - 1,)),
        ],
        compiler_params=pltpu.CompilerParams(
            collective_id=0, has_side_effects=True, vmem_limit_bytes=24 * 2**20
        ),
    )(*[pltpu.with_memory_space_constraint(array, pltpu.HBM) for array in arrays])
    return pl.pallas_call(
        finish,
        out_shape=(jax.ShapeDtypeStruct((LEV, COLS), F32), jax.ShapeDtypeStruct((NT, COLS), F32)),
        in_specs=[in_vmem] * 4,
        out_specs=(any_space, any_space),
        scratch_shapes=[tile_rows, pltpu.SemaphoreType.DMA((2,))],
        compiler_params=pltpu.CompilerParams(vmem_limit_bytes=4 * 2**20),
    )(*results)


def solution(mesh):
    columns, lines = P(None, ("lon", "lev")), P(("lon", "lev"))
    return jax.shard_map(
        on_device,
        mesh=mesh,
        in_specs=(columns, columns, lines, lines) + (columns,) * 6,
        out_specs=(columns, columns),
        check_vma=False,
    )
```

```python
import jax
import jax.numpy as jnp
from jax import lax
from jax.experimental import pallas as pl
from jax.experimental.pallas import tpu as pltpu
from jax.sharding import PartitionSpec as P

LEV = 70
NT = 9
COLS = 8192
ROWS = 64
LANES = 128
ITERS = 8
N_LON = 64
N_LEV = 4
N_Y = 4
N_Z = 8
MESH = pl.DeviceIdType.MESH
F32 = jnp.float32
BF16 = jnp.bfloat16
I32 = jnp.int32


def row(ref, level, start=0):
    return ref[pl.ds(level, 1), pl.ds(start, COLS)].reshape(ROWS, LANES)


def two_parts(value):
    high = value.astype(BF16)
    return jnp.concatenate([high, (value - high.astype(F32)).astype(BF16)], axis=1)


def take(value, index):
    return jnp.take_along_axis(value, index, axis=1, mode="promise_in_bounds")


def flag(condition):
    return jnp.where(condition, 1.0, 0.0).astype(BF16)


def iota(shape, dim):
    return lax.broadcasted_iota(I32, shape, dim)


def away(step, length):
    return min(step, length - step)


OFFSETS = sorted(
    [(dy, dz, other) for dy in range(N_Y) for dz in range(N_Z) for other in range(2) if dy + dz + other],
    key=lambda step: -(2 * away(step[0], N_Y) + 2 * away(step[1], N_Z) + step[2]),
)


def neighbours(lon):
    y, z, core = lon // (2 * N_Z), (lon // 2) % N_Z, lon % 2
    at_y = [(y + step) % N_Y * (2 * N_Z) for step in range(N_Y)]
    at_z = [(z + step) % N_Z * 2 for step in range(N_Z)]
    at_core = [core, 1 - core]
    return lambda dy, dz, other: at_y[dy] + at_z[dz] + at_core[other]


def exchange(send, recv, total, sems, peers, lon, lev):
    copies = [
        pltpu.make_async_remote_copy(
            src_ref=send.at[pl.ds(peer, 1), :], dst_ref=recv.at[pl.ds(lon, 1), :], send_sem=sems.at[0], recv_sem=sems.at[1],
            device_id={"lon": peer, "lev": lev}, device_id_type=MESH,
        )
        for peer in peers
    ]
    return copies, pltpu.make_async_remote_copy(
        src_ref=total, dst_ref=total, send_sem=sems.at[0], recv_sem=sems.at[1],
        device_id={"lon": peers[0], "lev": lev}, device_id_type=MESH,
    )


def solve(k_base, pivot_base, right_one, old_ground, column_a, column_b):
    flux = jnp.zeros_like(k_base)
    ground_a, one_b = old_ground + column_a, 1.0 + column_b
    for _ in range(ITERS):
        k_ground = k_base * (1.0 + 0.5 * jnp.tanh(flux))
        pivot_one = pivot_base + k_ground
        surface = (ground_a * pivot_one + k_ground * right_one) / (one_b * pivot_one + k_ground * pivot_base)
        flux = column_a - column_b * surface
    return surface, k_ground, pivot_one


def kernel(
    col_h, cpl_h, sea_h, mask_h, w_h, co_h, ca_h, cd_h, old_h, fo_h,
    out, land_out, scaled, coeff_r,
    col, cpl, ks, es, fs, sea_s, mask_s, w_s, co_s, ca_s, cd_s, old_s, fo_s,
    ab_send, ab_recv, to_land, from_columns,
    halo_out, halo_in, ab_total, land_total, in_sem, halo_send_sem, halo_recv_sem, ab_sems, land_sems, heard,
):
    lon, lev = lax.axis_index("lon"), lax.axis_index("lev")
    block = lon * N_LEV + lev
    right, left = (block + 1) % (N_LON * N_LEV), (block + N_LON * N_LEV - 1) % (N_LON * N_LEV)
    right_id = {"lon": right // N_LEV, "lev": right % N_LEV}
    left_id = {"lon": left // N_LEV, "lev": left % N_LEV}

    pairs = [
        (mask_h, mask_s), (co_h, co_s), (ca_h, ca_s), (cd_h, cd_s), (old_h, old_s), (fo_h, fo_s), (w_h, w_s), (cpl_h, cpl),
        (col_h, col), (sea_h, sea_s),
    ]
    loads = [pltpu.make_async_copy(src, dst, in_sem.at[n]) for n, (src, dst) in enumerate(pairs)]
    for load in loads:
        load.start()

    barrier = pltpu.get_barrier_semaphore()

    for one in (left_id, right_id):
        pl.semaphore_signal(barrier, inc=1, device_id=one, device_id_type=MESH)
    at = neighbours(lon)
    peers = [at(*offset) for offset in OFFSETS]
    ring = [at(*offset) for offset in OFFSETS if offset[0] == 0 and away(offset[1], N_Z) < N_Z // 2]
    rows_y = [at(step, 0, 0) for step in range(1, N_Y)]

    def tell(semaphore, device):
        pl.semaphore_signal(semaphore, inc=1, device_id={"lon": device, "lev": lev}, device_id_type=MESH)

    for device in ring + rows_y:
        tell(barrier, device)

    lane = iota((ROWS, LANES), 1)
    loads[0].wait()
    is_land = mask_s[...] == 1
    land = flag(is_land)
    running = jnp.dot(land, flag(iota((LANES, LANES), 0) <= iota((LANES, LANES), 1)), preferred_element_type=F32)
    count = jnp.dot(land, jnp.ones((LANES, LANES), BF16), preferred_element_type=F32)
    before = jnp.dot(
        flag(iota((ROWS, ROWS), 1) < iota((ROWS, ROWS), 0)), count.astype(BF16), preferred_element_type=F32
    ).astype(I32)
    running, count = running.astype(I32), count.astype(I32)
    first_window, shift = before >> 6, before & 63
    windows = [flag(lane == first_window + n) for n in range(3)]
    place = shift + running - 1
    window_of, slot_a = place >> 6, place & 63
    slot_b = slot_a + 64
    lane_of = jnp.zeros((ROWS, LANES), I32)
    for half in (64, 32, 16, 8, 4, 2, 1):
        seen = take(running, lane_of + (half - 1))
        lane_of = jnp.where(seen <= lane, lane_of + half, lane_of)
    turned = (lane - shift) & 127
    lane_of = take(lane_of, turned)
    used = turned < count
    in_front, behind = used & (lane >= shift), used & (lane < shift)
    line = iota((ROWS, LANES), 0)
    last = jnp.broadcast_to((before + count)[ROWS - 1 :, :], (ROWS, LANES)) - 1
    last_flag = jnp.broadcast_to(mask_s[pl.ds(ROWS - 1, 1), :][:, LANES - 1 :], (ROWS, LANES))
    first_column, last_column = (line == 0) & (lane == 0), (line == ROWS - 1) & (lane == LANES - 1)
    first_slot = first_column & is_land
    last_slot = (line == (last & 63)) & (lane == (last >> 6)) & (last_flag == 1)

    for load in loads[1:7]:
        load.wait()

    weight_sum = sum_a = sum_b = None
    for tile in range(NT):
        weight, coeff = row(w_s, tile), row(co_s, tile)
        capacity, conduct = row(ca_s, tile), row(cd_s, tile)
        held = capacity + conduct
        inverse = 1.0 / (capacity + coeff + conduct)
        source = capacity * row(old_s, tile) + row(fo_s, tile)
        ratio = coeff * inverse
        scaled[tile] = source * inverse
        coeff_r[tile] = ratio
        share = weight * ratio
        weight_sum = weight if tile == 0 else weight_sum + weight
        sum_a = share * source if tile == 0 else sum_a + share * source
        sum_b = share * held if tile == 0 else sum_b + share * held
    whole = 1.0 / weight_sum
    ab_send[:, pl.ds(0, LANES)] = sum_a * whole
    ab_send[:, pl.ds(LANES, LANES)] = sum_b * whole
    loads[7].wait()

    lane_wide = iota((LEV - 1, LANES), 1)
    diagonal = iota((LEV - 1, LANES), 0) == lane_wide

    def as_row(column):
        wide = jnp.broadcast_to(column, (LEV - 1, LANES))
        return jnp.sum(jnp.where(diagonal, wide, 0.0), axis=0, keepdims=True)

    def as_column(line):
        wide = jnp.broadcast_to(line, (LEV - 1, LANES))
        return jnp.sum(jnp.where(diagonal, wide, 0.0), axis=1, keepdims=True)

    halo_out[pl.ds(0, 1), :] = as_row(cpl[:, pl.ds(COLS - LANES, LANES)][:, LANES - 1 :])
    halo_out[pl.ds(8, 1), :] = as_row(cpl[:, pl.ds(0, LANES)][:, :1])
    pl.semaphore_wait(barrier, len(ring) + len(rows_y) + 2)

    halos = [
        pltpu.make_async_remote_copy(
            src_ref=halo_out.at[pl.ds(line, 1), :], dst_ref=halo_in.at[pl.ds(line, 1), :],
            send_sem=halo_send_sem.at[n], recv_sem=halo_recv_sem.at[n], device_id=device, device_id_type=MESH,
        )
        for n, (line, device) in enumerate(((0, right_id), (8, left_id)))
    ]
    for halo in halos:
        halo.start()
    for step, device in enumerate(rows_y):
        tell(heard.at[1 + step], device)

    def smooth(chunk, left=None, right=None):
        centre = cpl[:, pl.ds(chunk * LANES, LANES)]
        if left is None:
            below = cpl[:, pl.ds((chunk - 1) * LANES, LANES)]
            low = pltpu.roll(jnp.where(lane_wide == LANES - 1, below, centre), 1, 1)
        else:
            low = jnp.where(lane_wide == 0, left, pltpu.roll(centre, 1, 1))
        if right is None:
            above = cpl[:, pl.ds((chunk + 1) * LANES, LANES)]
            high = pltpu.roll(jnp.where(lane_wide == 0, above, centre), LANES - 1, 1)
        else:
            high = jnp.where(lane_wide == LANES - 1, right, pltpu.roll(centre, LANES - 1, 1))
        ks[:, pl.ds(chunk * LANES, LANES)] = (low + 2.0 * centre + high) * 0.25

    smooth(0, left=0.0)
    smooth(ROWS - 1, right=0.0)
    for chunk in range(1, ROWS - 1):
        smooth(chunk)
    for step in range(len(rows_y)):
        pl.semaphore_wait(heard.at[1 + step], 1)
    tell(heard.at[0], at(0, N_Z - 1, 0))
    ab_out, ab_all = exchange(ab_send, ab_recv, ab_total, ab_sems, peers, lon, lev)
    for offset, copy in zip(OFFSETS, ab_out):
        if offset[1] != N_Z // 2:
            copy.start()
    ab_recv[pl.ds(lon, 1), :] = ab_send[pl.ds(lon, 1), :]

    def eliminate(level, carried, k_row, old_row, keep):
        k_here, offset, top, bottom = carried
        k_below = k_row(level - 1)
        part = k_below * bottom
        pivot = part + top
        inverse = 1.0 / pivot
        offset = (old_row(level) + k_here * offset) * (bottom * inverse)
        keep(level, offset, part * inverse)
        return (k_below, offset, part + (1.0 + k_below) * top, pivot), inverse

    def scaled_down(carried, inverse):
        k_here, offset, top, _ = carried
        return k_here, offset, top * inverse, jnp.ones_like(top)

    def start_of(shape):
        zeros, ones = jnp.zeros(shape, F32), jnp.ones(shape, F32)
        return zeros, zeros, ones, ones

    def keep_all(level, offset, factor):
        es[level] = offset
        fs[level] = factor

    def all_columns(step, carried):
        for n in range(4):
            carried, inverse = eliminate(
                LEV - 1 - 4 * step - n, carried, lambda level: row(ks, level), lambda level: row(col, level), keep_all
            )
        return scaled_down(carried, inverse)

    loads[8].wait()
    k_second, offset_two, pivot_base, _ = lax.fori_loop(0, (LEV - 2) // 4, all_columns, start_of((ROWS, LANES)))
    fields = [row(ks, 0), pivot_base, row(col, 1) + k_second * offset_two, row(col, 0)]

    pl.semaphore_wait(heard.at[0], 1)
    for offset, copy in zip(OFFSETS, ab_out):
        if offset[1] == N_Z // 2:
            copy.start()

    targets = jnp.concatenate(
        [
            jnp.concatenate([windows[0], windows[2]], axis=0),
            jnp.concatenate([windows[1], jnp.zeros((ROWS, LANES), BF16)], axis=0),
        ],
        axis=1,
    )
    turned_fields = []
    for field in fields:
        ordered = take(jnp.where(first_column | last_column, 0.0, field), lane_of)
        turned_fields.append(
            jnp.concatenate([jnp.where(in_front, ordered, 0.0), jnp.where(behind, ordered, 0.0)], axis=0).T
        )
    placed = jnp.dot(
        two_parts(jnp.concatenate(turned_fields, axis=0)), jnp.concatenate([targets] * 2, axis=0),
        preferred_element_type=F32,
    )
    for n in range(len(fields)):
        top = 2 * ROWS * n
        to_land[:, pl.ds(n * LANES, LANES)] = (
            placed[top : top + ROWS, :LANES] + placed[top + ROWS : top + 2 * ROWS, LANES:]
        )

    for halo in halos:
        halo.wait_recv()
    smooth(0, left=as_column(halo_in[pl.ds(0, 1), :]))
    smooth(ROWS - 1, right=as_column(halo_in[pl.ds(8, 1), :]))
    sublane = iota((8, LANES), 0)

    def edge_row(ref, level):
        low, high = (ref[pl.ds(level, 1), pl.ds(start, 8 * LANES)].reshape(8, LANES) for start in (0, COLS - 8 * LANES))
        return jnp.where(sublane == 0, low, high)

    def keep_edges(level, offset, factor):
        for ref, value in ((es, offset), (fs, factor)):
            ref[level, pl.ds(0, 1), :] = value[0:1]
            ref[level, pl.ds(ROWS - 1, 1), :] = value[7:8]

    edge = start_of((8, LANES))
    for level in range(LEV - 1, 1, -1):
        edge, inverse = eliminate(
            level, edge, lambda level: edge_row(ks, level), lambda level: edge_row(col, level), keep_edges
        )
        if level % 12 == 2:
            edge = scaled_down(edge, inverse)
    edge_fields = [edge_row(ks, 0), edge[2], edge_row(col, 1) + edge[0] * edge[1], edge_row(col, 0)]

    for n, value in enumerate(edge_fields):
        part = pl.ds(n * LANES, LANES)
        first_value, last_value = value[0:1, 0:1], value[7:8, LANES - 1 :]
        to_land[:, part] = jnp.where(first_slot, first_value, jnp.where(last_slot, last_value, to_land[:, part]))
    land_outgoing, land_all = exchange(to_land, from_columns, land_total, land_sems, peers, lon, lev)
    for copy in land_outgoing:
        copy.start()
    from_columns[pl.ds(lon, 1), :] = to_land[pl.ds(lon, 1), :]
    loads[9].wait()

    def joined(all_rows, edges):
        first = jnp.where(sublane == 0, edges, all_rows[0:8])
        last_rows = jnp.where(sublane == 7, edges, all_rows[ROWS - 8 :])
        return jnp.concatenate([first, all_rows[8 : ROWS - 8], last_rows], axis=0)

    fields = [joined(field, edges) for field, edges in zip(fields, edge_fields)]
    right_one = fields[2]

    ab_all.wait_recv()
    both = jnp.concatenate([ab_recv[:, pl.ds(0, LANES)], ab_recv[:, pl.ds(LANES, LANES)]], axis=0)
    stacked = jnp.concatenate(windows, axis=0)
    picked = lax.dot_general(
        jnp.concatenate([stacked] * 2, axis=1), two_parts(both),
        (((1,), (1,)), ((), ())), preferred_element_type=F32,
    )
    pieces = [picked[n * ROWS : (n + 1) * ROWS] for n in range(3)]

    def unpack(slot):
        found = [take(piece, slot) for piece in pieces]
        return jnp.where(window_of == 0, found[0], jnp.where(window_of == 1, found[1], found[2]))

    column_a = jnp.where(is_land, unpack(slot_a), sea_s[...])
    column_b = jnp.where(is_land, unpack(slot_b), 1.0)

    surface, k_ground, pivot_one = solve(*fields, column_a, column_b)
    inverse = 1.0 / pivot_one
    offset_one, factor_one = right_one * inverse, k_ground * inverse

    value = offset_one + factor_one * surface
    out[pl.ds(0, 1), :] = surface.reshape(1, COLS)
    out[pl.ds(1, 1), :] = value.reshape(1, COLS)
    for level in range(2, LEV):
        value = es[level] + fs[level] * value
        out[pl.ds(level, 1), :] = value.reshape(1, COLS)

    for copy in (*halos, ab_all, land_all):
        copy.wait_send()
    land_all.wait_recv()
    land_out[:, pl.ds(0, 4 * LANES)] = from_columns[...]
    land_out[:, pl.ds(4 * LANES, 2 * LANES)] = ab_send[...]


def finish(out, land, scaled, coeff_r, out_h, tile_h, tile_o, sems):
    stores = [pltpu.make_async_copy(out, out_h, sems.at[0]), pltpu.make_async_copy(tile_o, tile_h, sems.at[1])]
    stores[0].start()
    k_base, pivot_base, right_one, old_ground, land_a, land_b = (land[:, pl.ds(n * LANES, LANES)] for n in range(6))
    taken = pivot_base > 0.0
    surface, _, _ = solve(k_base, jnp.where(taken, pivot_base, 1.0), right_one, old_ground, land_a, land_b)
    land_surface = jnp.where(taken, surface, 0.0)
    for tile in range(NT):
        tile_o[pl.ds(tile, 1), :] = (scaled[tile] + coeff_r[tile] * land_surface).reshape(1, COLS)
    stores[1].start()
    for store in stores:
        store.wait()


def on_device(column_old, coupling, sea_temp, land_mask, *tiles):
    any_space = pl.BlockSpec(memory_space=pl.ANY)
    levels, tile_rows = pltpu.VMEM((LEV, COLS), F32), pltpu.VMEM((NT, COLS), F32)
    plane = pltpu.VMEM((ROWS, LANES), F32)
    in_vmem = pl.BlockSpec(memory_space=pltpu.VMEM)
    arrays = (column_old, coupling, sea_temp.reshape(ROWS, LANES), land_mask.reshape(ROWS, LANES), *tiles)
    tile_planes = pltpu.VMEM((NT, ROWS, LANES), F32)
    results = pl.pallas_call(
        kernel,
        out_shape=(levels, pltpu.VMEM((ROWS, 6 * LANES), F32), tile_planes, tile_planes),
        in_specs=[any_space] * 10,
        out_specs=(in_vmem,) * 4,
        scratch_shapes=[
            levels,
            pltpu.VMEM((LEV - 1, COLS), F32),
            pltpu.VMEM((LEV - 1, COLS), F32),
            pltpu.VMEM((LEV, ROWS, LANES), F32),
            pltpu.VMEM((LEV, ROWS, LANES), F32),
            plane,
            pltpu.VMEM((ROWS, LANES), I32),
            *[tile_rows] * 6,
            *[pltpu.VMEM((N_LON, 2 * LANES), F32)] * 2,
            *[pltpu.VMEM((N_LON, 4 * LANES), F32)] * 2,
            *[pltpu.VMEM((16, LANES), F32)] * 2,
            pltpu.VMEM(((N_LON - 1) * 2, LANES), F32),
            pltpu.VMEM(((N_LON - 1) * 4, LANES), F32),
            pltpu.SemaphoreType.DMA((10,)),
            pltpu.SemaphoreType.DMA((2,)),
            pltpu.SemaphoreType.DMA((2,)),
            pltpu.SemaphoreType.DMA((2,)),
            pltpu.SemaphoreType.DMA((2,)),
            pltpu.SemaphoreType.REGULAR((N_Y,)),
        ],
        compiler_params=pltpu.CompilerParams(
            collective_id=0, has_side_effects=True, vmem_limit_bytes=24 * 2**20
        ),
    )(*[pltpu.with_memory_space_constraint(array, pltpu.HBM) for array in arrays])
    return pl.pallas_call(
        finish,
        out_shape=(jax.ShapeDtypeStruct((LEV, COLS), F32), jax.ShapeDtypeStruct((NT, COLS), F32)),
        in_specs=[in_vmem] * 4,
        out_specs=(any_space, any_space),
        scratch_shapes=[tile_rows, pltpu.SemaphoreType.DMA((2,))],
        compiler_params=pltpu.CompilerParams(vmem_limit_bytes=4 * 2**20),
    )(*results)


def solution(mesh):
    columns, lines = P(None, ("lon", "lev")), P(("lon", "lev"))
    return jax.shard_map(
        on_device,
        mesh=mesh,
        in_specs=(columns, columns, lines, lines) + (columns,) * 6,
        out_specs=(columns, columns),
        check_vma=False,
    )
```

```python
import jax
import jax.numpy as jnp
from jax import lax
from jax.experimental import pallas as pl
from jax.experimental.pallas import tpu as pltpu
from jax.sharding import PartitionSpec as P

LEV = 70
NT = 9
COLS = 8192
ROWS = 64
LANES = 128
ITERS = 8
N_LON = 64
N_LEV = 4
N_Y = 4
N_Z = 8
MESH = pl.DeviceIdType.MESH
F32 = jnp.float32
BF16 = jnp.bfloat16
I32 = jnp.int32


def row(ref, level, start=0):
    return ref[pl.ds(level, 1), pl.ds(start, COLS)].reshape(ROWS, LANES)


def two_parts(value):
    high = value.astype(BF16)
    return jnp.concatenate([high, (value - high.astype(F32)).astype(BF16)], axis=1)


def take(value, index):
    return jnp.take_along_axis(value, index, axis=1, mode="promise_in_bounds")


def flag(condition):
    return jnp.where(condition, 1.0, 0.0).astype(BF16)


def iota(shape, dim):
    return lax.broadcasted_iota(I32, shape, dim)


def away(step, length):
    return min(step, length - step)


OFFSETS = sorted(
    [(dy, dz, other) for dy in range(N_Y) for dz in range(N_Z) for other in range(2) if dy + dz + other],
    key=lambda step: -(2 * away(step[0], N_Y) + 2 * away(step[1], N_Z) + step[2]),
)


def neighbours(lon):
    y, z, core = lon // (2 * N_Z), (lon // 2) % N_Z, lon % 2
    at_y = [(y + step) % N_Y * (2 * N_Z) for step in range(N_Y)]
    at_z = [(z + step) % N_Z * 2 for step in range(N_Z)]
    at_core = [core, 1 - core]
    return lambda dy, dz, other: at_y[dy] + at_z[dz] + at_core[other]


def exchange(send, recv, total, sems, peers, lon, lev):
    copies = [
        pltpu.make_async_remote_copy(
            src_ref=send.at[pl.ds(peer, 1), :], dst_ref=recv.at[pl.ds(lon, 1), :], send_sem=sems.at[0], recv_sem=sems.at[1],
            device_id={"lon": peer, "lev": lev}, device_id_type=MESH,
        )
        for peer in peers
    ]
    return copies, pltpu.make_async_remote_copy(
        src_ref=total, dst_ref=total, send_sem=sems.at[0], recv_sem=sems.at[1],
        device_id={"lon": peers[0], "lev": lev}, device_id_type=MESH,
    )


def solve(k_base, pivot_base, right_one, old_ground, column_a, column_b):
    flux = jnp.zeros_like(k_base)
    ground_a, one_b = old_ground + column_a, 1.0 + column_b
    for _ in range(ITERS):
        k_ground = k_base * (1.0 + 0.5 * jnp.tanh(flux))
        pivot_one = pivot_base + k_ground
        surface = (ground_a * pivot_one + k_ground * right_one) / (one_b * pivot_one + k_ground * pivot_base)
        flux = column_a - column_b * surface
    return surface, k_ground, pivot_one


def kernel(
    col_h, cpl_h, sea_h, mask_h, w_h, co_h, ca_h, cd_h, old_h, fo_h,
    out, land_out, scaled, coeff_r,
    col, cpl, ks, es, fs, sea_s, mask_s, w_s, co_s, ca_s, cd_s, old_s, fo_s,
    ab_send, ab_recv, to_land, from_columns,
    halo_out, halo_in, missing, ab_total, land_total, in_sem, halo_send_sem, halo_recv_sem, ab_sems, land_sems, heard,
):
    lon, lev = lax.axis_index("lon"), lax.axis_index("lev")
    block = lon * N_LEV + lev
    right, left = (block + 1) % (N_LON * N_LEV), (block + N_LON * N_LEV - 1) % (N_LON * N_LEV)
    right_id = {"lon": right // N_LEV, "lev": right % N_LEV}
    left_id = {"lon": left // N_LEV, "lev": left % N_LEV}

    pairs = [
        (mask_h, mask_s), (co_h, co_s), (ca_h, ca_s), (cd_h, cd_s), (old_h, old_s), (fo_h, fo_s), (w_h, w_s), (cpl_h, cpl),
        (col_h, col), (sea_h, sea_s),
    ]
    barrier = pltpu.get_barrier_semaphore()

    for one in (left_id, right_id):
        pl.semaphore_signal(barrier, inc=1, device_id=one, device_id_type=MESH)
    at = neighbours(lon)
    peers = [at(*offset) for offset in OFFSETS]
    ring = [at(*offset) for offset in OFFSETS if offset[0] == 0 and away(offset[1], N_Z) < N_Z // 2]
    rows_y = [at(step, 0, 0) for step in range(1, N_Y)]

    def tell(semaphore, device):
        pl.semaphore_signal(semaphore, inc=1, device_id={"lon": device, "lev": lev}, device_id_type=MESH)

    for device in ring + rows_y:
        tell(barrier, device)

    loads = [pltpu.make_async_copy(src, dst, in_sem.at[n]) for n, (src, dst) in enumerate(pairs)]
    for load in loads:
        load.start()

    lane = iota((ROWS, LANES), 1)
    loads[0].wait()
    is_land = mask_s[...] == 1
    land = flag(is_land)
    running = jnp.dot(land, flag(iota((LANES, LANES), 0) <= iota((LANES, LANES), 1)), preferred_element_type=F32)
    count = jnp.dot(land, jnp.ones((LANES, LANES), BF16), preferred_element_type=F32)
    before = jnp.dot(
        flag(iota((ROWS, ROWS), 1) < iota((ROWS, ROWS), 0)), count.astype(BF16), preferred_element_type=F32
    ).astype(I32)
    running, count = running.astype(I32), count.astype(I32)
    first_window, shift = before >> 6, before & 63
    windows = [flag(lane == first_window + n) for n in range(3)]
    place = shift + running - 1
    window_of, slot_a = place >> 6, place & 63
    slot_b = slot_a + 64
    lane_of = jnp.zeros((ROWS, LANES), I32)
    for half in (64, 32, 16, 8, 4, 2, 1):
        seen = take(running, lane_of + (half - 1))
        lane_of = jnp.where(seen <= lane, lane_of + half, lane_of)
    turned = (lane - shift) & 127
    lane_of = take(lane_of, turned)
    used = turned < count
    in_front, behind = used & (lane >= shift), used & (lane < shift)
    line = iota((ROWS, LANES), 0)
    last = jnp.broadcast_to((before + count)[ROWS - 1 :, :], (ROWS, LANES)) - 1
    last_flag = jnp.broadcast_to(mask_s[pl.ds(ROWS - 1, 1), :][:, LANES - 1 :], (ROWS, LANES))
    first_column, last_column = (line == 0) & (lane == 0), (line == ROWS - 1) & (lane == LANES - 1)
    first_slot = first_column & is_land
    last_slot = (line == (last & 63)) & (lane == (last >> 6)) & (last_flag == 1)

    for load in loads[1:7]:
        load.wait()

    weight_sum = sum_a = sum_b = None
    for tile in range(NT):
        weight, coeff = row(w_s, tile), row(co_s, tile)
        capacity, conduct = row(ca_s, tile), row(cd_s, tile)
        held = capacity + conduct
        inverse = 1.0 / (capacity + coeff + conduct)
        source = capacity * row(old_s, tile) + row(fo_s, tile)
        ratio = coeff * inverse
        scaled[tile] = source * inverse
        coeff_r[tile] = ratio
        share = weight * ratio
        weight_sum = weight if tile == 0 else weight_sum + weight
        sum_a = share * source if tile == 0 else sum_a + share * source
        sum_b = share * held if tile == 0 else sum_b + share * held
    whole = 1.0 / weight_sum
    ab_send[:, pl.ds(0, LANES)] = sum_a * whole
    ab_send[:, pl.ds(LANES, LANES)] = sum_b * whole
    loads[7].wait()

    lane_wide = iota((LEV - 1, LANES), 1)
    diagonal = iota((LEV - 1, LANES), 0) == lane_wide

    def as_row(column):
        wide = jnp.broadcast_to(column, (LEV - 1, LANES))
        return jnp.sum(jnp.where(diagonal, wide, 0.0), axis=0, keepdims=True)

    def as_column(line):
        wide = jnp.broadcast_to(line, (LEV - 1, LANES))
        return jnp.sum(jnp.where(diagonal, wide, 0.0), axis=1, keepdims=True)

    halo_out[pl.ds(0, 1), :] = as_row(cpl[:, pl.ds(COLS - LANES, LANES)][:, LANES - 1 :])
    halo_out[pl.ds(8, 1), :] = as_row(cpl[:, pl.ds(0, LANES)][:, :1])
    pl.semaphore_wait(barrier, len(ring) + len(rows_y) + 2)

    halos = [
        pltpu.make_async_remote_copy(
            src_ref=halo_out.at[pl.ds(line, 1), :], dst_ref=halo_in.at[pl.ds(line, 1), :],
            send_sem=halo_send_sem.at[n], recv_sem=halo_recv_sem.at[n], device_id=device, device_id_type=MESH,
        )
        for n, (line, device) in enumerate(((0, right_id), (8, left_id)))
    ]
    for halo in halos:
        halo.start()
    for step, device in enumerate(rows_y):
        tell(heard.at[1 + step], device)

    def smooth(chunk, left=None, right=None):
        centre = cpl[:, pl.ds(chunk * LANES, LANES)]
        if left is None:
            below = cpl[:, pl.ds((chunk - 1) * LANES, LANES)]
            low = pltpu.roll(jnp.where(lane_wide == LANES - 1, below, centre), 1, 1)
        else:
            low = jnp.where(lane_wide == 0, left, pltpu.roll(centre, 1, 1))
        if right is None:
            above = cpl[:, pl.ds((chunk + 1) * LANES, LANES)]
            high = pltpu.roll(jnp.where(lane_wide == 0, above, centre), LANES - 1, 1)
        else:
            high = jnp.where(lane_wide == LANES - 1, right, pltpu.roll(centre, LANES - 1, 1))
        ks[:, pl.ds(chunk * LANES, LANES)] = (low + 2.0 * centre + high) * 0.25

    smooth(0, left=0.0)
    smooth(ROWS - 1, right=0.0)
    for chunk in range(1, ROWS - 1):
        smooth(chunk)
    for step in range(len(rows_y)):
        pl.semaphore_wait(heard.at[1 + step], 1)
    tell(heard.at[0], at(0, N_Z - 1, 0))
    ab_out, ab_all = exchange(ab_send, ab_recv, ab_total, ab_sems, peers, lon, lev)
    for offset, copy in zip(OFFSETS, ab_out):
        if offset[1] != N_Z // 2:
            copy.start()
    ab_recv[pl.ds(lon, 1), :] = ab_send[pl.ds(lon, 1), :]

    def eliminate(level, carried, k_row, old_row, keep):
        k_here, offset, top, bottom = carried
        k_below = k_row(level - 1)
        part = k_below * bottom
        pivot = part + top
        inverse = 1.0 / pivot
        offset = (old_row(level) + k_here * offset) * (bottom * inverse)
        keep(level, offset, part * inverse)
        return (k_below, offset, part + (1.0 + k_below) * top, pivot), inverse

    def scaled_down(carried, inverse):
        k_here, offset, top, _ = carried
        return k_here, offset, top * inverse, jnp.ones_like(top)

    def start_of(shape):
        zeros, ones = jnp.zeros(shape, F32), jnp.ones(shape, F32)
        return zeros, zeros, ones, ones

    def keep_all(level, offset, factor):
        es[level] = offset
        fs[level] = factor

    def all_columns(step, carried):
        for n in range(4):
            carried, inverse = eliminate(
                LEV - 1 - 4 * step - n, carried, lambda level: row(ks, level), lambda level: row(col, level), keep_all
            )
        return scaled_down(carried, inverse)

    loads[8].wait()
    k_second, offset_two, pivot_base, _ = lax.fori_loop(0, (LEV - 2) // 4, all_columns, start_of((ROWS, LANES)))
    fields = [row(ks, 0), pivot_base, row(col, 1) + k_second * offset_two, row(col, 0)]

    pl.semaphore_wait(heard.at[0], 1)
    for offset, copy in zip(OFFSETS, ab_out):
        if offset[1] == N_Z // 2:
            copy.start()

    targets = jnp.concatenate(
        [
            jnp.concatenate([windows[0], windows[2]], axis=0),
            jnp.concatenate([windows[1], jnp.zeros((ROWS, LANES), BF16)], axis=0),
        ],
        axis=1,
    )
    turned_fields = []
    for field in fields:
        ordered = take(jnp.where(first_column | last_column, 0.0, field), lane_of)
        turned_fields.append(
            jnp.concatenate([jnp.where(in_front, ordered, 0.0), jnp.where(behind, ordered, 0.0)], axis=0).T
        )
    placed = jnp.dot(
        two_parts(jnp.concatenate(turned_fields, axis=0)), jnp.concatenate([targets] * 2, axis=0),
        preferred_element_type=F32,
    )
    for n in range(len(fields)):
        top = 2 * ROWS * n
        to_land[:, pl.ds(n * LANES, LANES)] = (
            placed[top : top + ROWS, :LANES] + placed[top + ROWS : top + 2 * ROWS, LANES:]
        )

    for halo in halos:
        halo.wait_recv()
    missing[...] = 0.25 * jnp.where(
        lane_wide == 0, as_column(halo_in[pl.ds(0, 1), :]),
        jnp.where(lane_wide == LANES - 1, as_column(halo_in[pl.ds(8, 1), :]), 0.0),
    )
    sublane, edge_lane = iota((8, LANES), 0), iota((8, LANES), 1)
    corners = ((sublane == 0) & (edge_lane == 0)) | ((sublane == 7) & (edge_lane == LANES - 1))

    def edge_row(ref, level):
        low, high = (ref[pl.ds(level, 1), pl.ds(start, 8 * LANES)].reshape(8, LANES) for start in (0, COLS - 8 * LANES))
        return jnp.where(sublane == 0, low, high)

    def edge_smooth(level):
        return edge_row(ks, level) + jnp.where(corners, missing[pl.ds(level, 1), :], 0.0)

    def keep_edges(level, offset, factor):
        for ref, value in ((es, offset), (fs, factor)):
            ref[level, pl.ds(0, 1), :] = value[0:1]
            ref[level, pl.ds(ROWS - 1, 1), :] = value[7:8]

    edge = start_of((8, LANES))
    for level in range(LEV - 1, 1, -1):
        edge, inverse = eliminate(
            level, edge, edge_smooth, lambda level: edge_row(col, level), keep_edges
        )
        if level % 12 == 2:
            edge = scaled_down(edge, inverse)
    edge_fields = [edge_smooth(0), edge[2], edge_row(col, 1) + edge[0] * edge[1], edge_row(col, 0)]

    for n, value in enumerate(edge_fields):
        part = pl.ds(n * LANES, LANES)
        first_value, last_value = value[0:1, 0:1], value[7:8, LANES - 1 :]
        to_land[:, part] = jnp.where(first_slot, first_value, jnp.where(last_slot, last_value, to_land[:, part]))
    land_outgoing, land_all = exchange(to_land, from_columns, land_total, land_sems, peers, lon, lev)
    for copy in land_outgoing:
        copy.start()
    from_columns[pl.ds(lon, 1), :] = to_land[pl.ds(lon, 1), :]
    loads[9].wait()

    def joined(all_rows, edges):
        first = jnp.where(sublane == 0, edges, all_rows[0:8])
        last_rows = jnp.where(sublane == 7, edges, all_rows[ROWS - 8 :])
        return jnp.concatenate([first, all_rows[8 : ROWS - 8], last_rows], axis=0)

    fields = [joined(field, edges) for field, edges in zip(fields, edge_fields)]
    right_one = fields[2]

    ab_all.wait_recv()
    both = jnp.concatenate([ab_recv[:, pl.ds(0, LANES)], ab_recv[:, pl.ds(LANES, LANES)]], axis=0)
    stacked = jnp.concatenate(windows, axis=0)
    picked = lax.dot_general(
        jnp.concatenate([stacked] * 2, axis=1), two_parts(both),
        (((1,), (1,)), ((), ())), preferred_element_type=F32,
    )
    pieces = [picked[n * ROWS : (n + 1) * ROWS] for n in range(3)]

    def unpack(slot):
        found = [take(piece, slot) for piece in pieces]
        return jnp.where(window_of == 0, found[0], jnp.where(window_of == 1, found[1], found[2]))

    column_a = jnp.where(is_land, unpack(slot_a), sea_s[...])
    column_b = jnp.where(is_land, unpack(slot_b), 1.0)

    surface, k_ground, pivot_one = solve(*fields, column_a, column_b)
    inverse = 1.0 / pivot_one
    offset_one, factor_one = right_one * inverse, k_ground * inverse

    value = offset_one + factor_one * surface
    out[pl.ds(0, 1), :] = surface.reshape(1, COLS)
    out[pl.ds(1, 1), :] = value.reshape(1, COLS)
    for level in range(2, LEV):
        value = es[level] + fs[level] * value
        out[pl.ds(level, 1), :] = value.reshape(1, COLS)

    for copy in (*halos, ab_all, land_all):
        copy.wait_send()
    land_all.wait_recv()
    land_out[:, pl.ds(0, 4 * LANES)] = from_columns[...]
    land_out[:, pl.ds(4 * LANES, 2 * LANES)] = ab_send[...]


def finish(out, land, scaled, coeff_r, out_h, tile_h, tile_o, sems):
    stores = [pltpu.make_async_copy(out, out_h, sems.at[0]), pltpu.make_async_copy(tile_o, tile_h, sems.at[1])]
    stores[0].start()
    k_base, pivot_base, right_one, old_ground, land_a, land_b = (land[:, pl.ds(n * LANES, LANES)] for n in range(6))
    taken = pivot_base > 0.0
    surface, _, _ = solve(k_base, jnp.where(taken, pivot_base, 1.0), right_one, old_ground, land_a, land_b)
    land_surface = jnp.where(taken, surface, 0.0)
    for tile in range(NT):
        tile_o[pl.ds(tile, 1), :] = (scaled[tile] + coeff_r[tile] * land_surface).reshape(1, COLS)
    stores[1].start()
    for store in stores:
        store.wait()


def on_device(column_old, coupling, sea_temp, land_mask, *tiles):
    any_space = pl.BlockSpec(memory_space=pl.ANY)
    levels, tile_rows = pltpu.VMEM((LEV, COLS), F32), pltpu.VMEM((NT, COLS), F32)
    plane = pltpu.VMEM((ROWS, LANES), F32)
    in_vmem = pl.BlockSpec(memory_space=pltpu.VMEM)
    arrays = (column_old, coupling, sea_temp.reshape(ROWS, LANES), land_mask.reshape(ROWS, LANES), *tiles)
    tile_planes = pltpu.VMEM((NT, ROWS, LANES), F32)
    results = pl.pallas_call(
        kernel,
        out_shape=(levels, pltpu.VMEM((ROWS, 6 * LANES), F32), tile_planes, tile_planes),
        in_specs=[any_space] * 10,
        out_specs=(in_vmem,) * 4,
        scratch_shapes=[
            levels,
            pltpu.VMEM((LEV - 1, COLS), F32),
            pltpu.VMEM((LEV - 1, COLS), F32),
            pltpu.VMEM((LEV, ROWS, LANES), F32),
            pltpu.VMEM((LEV, ROWS, LANES), F32),
            plane,
            pltpu.VMEM((ROWS, LANES), I32),
            *[tile_rows] * 6,
            *[pltpu.VMEM((N_LON, 2 * LANES), F32)] * 2,
            *[pltpu.VMEM((N_LON, 4 * LANES), F32)] * 2,
            *[pltpu.VMEM((16, LANES), F32)] * 2,
            pltpu.VMEM((LEV - 1, LANES), F32),
            pltpu.VMEM(((N_LON - 1) * 2, LANES), F32),
            pltpu.VMEM(((N_LON - 1) * 4, LANES), F32),
            pltpu.SemaphoreType.DMA((10,)),
            pltpu.SemaphoreType.DMA((2,)),
            pltpu.SemaphoreType.DMA((2,)),
            pltpu.SemaphoreType.DMA((2,)),
            pltpu.SemaphoreType.DMA((2,)),
            pltpu.SemaphoreType.REGULAR((N_Y,)),
        ],
        compiler_params=pltpu.CompilerParams(
            collective_id=0, has_side_effects=True, vmem_limit_bytes=24 * 2**20
        ),
    )(*[pltpu.with_memory_space_constraint(array, pltpu.HBM) for array in arrays])
    return pl.pallas_call(
        finish,
        out_shape=(jax.ShapeDtypeStruct((LEV, COLS), F32), jax.ShapeDtypeStruct((NT, COLS), F32)),
        in_specs=[in_vmem] * 4,
        out_specs=(any_space, any_space),
        scratch_shapes=[tile_rows, pltpu.SemaphoreType.DMA((2,))],
        compiler_params=pltpu.CompilerParams(vmem_limit_bytes=4 * 2**20),
    )(*results)


def solution(mesh):
    columns, lines = P(None, ("lon", "lev")), P(("lon", "lev"))
    return jax.shard_map(
        on_device,
        mesh=mesh,
        in_specs=(columns, columns, lines, lines) + (columns,) * 6,
        out_specs=(columns, columns),
        check_vma=False,
    )
```
